32 devices in a mesh: blk: 8 (over z, y), grp: 4 (over x, core).
Axes of the slice: x: 2, y: 2, z: 4, core: 2. Of those that a mesh axis runs over, the one named last changes fastest.
Arguments:
- image_emb: bfloat16 [12288, 1152], P(('blk', 'grp')), may hold values from -0.1875 to 0.1875
- text_emb: bfloat16 [12288, 1152], P(('blk', 'grp')), may hold values from -0.1875 to 0.1875
- positives: int32 [32, 384], P(('blk', 'grp')), may hold values from 0 to 383, each once within a row
- pair_mask: int32 [8, 7], replicated, may hold values from 0 to 1, as said below
- log_scale: float32 [1], replicated, may hold values from 1.5 to 2.5
- bias: float32 [1], replicated, may hold values from -3 to -1
Outputs:
- image_grad: bfloat16 [12288, 1152], P(('blk', 'grp'))
- text_grad: bfloat16 [12288, 1152], P(('blk', 'grp'))
- loss: float32 [1], replicated
The draws below stay inside these ranges and needn't reach their ends.
Inputs may be any that keep to these rules, and one draw needn't show every extreme that they name: `positives`: every row is a permutation of the rows of a block. `pair_mask`: column 3 is 1 in every row (each image block is scored against its own text block); at least one row is all ones.
All inputs are finite; a program needn't handle non-finite values.
Results may differ from the reference program's by a relative error of at most 0.0063.
Values may be sent and summed in bfloat16 or wider, within the bound.
A program may use at most 64 MiB of HBM per device.

```python
import jax
import jax.numpy as jnp
from jax import lax

D = 1152
ROWS = 384
REACH = 3
IMAGES = 12288
N_BLK = 8
N_GRP = 4


def draw_pair_mask(key, part):
    first_key = jax.random.fold_in(key, 11)
    second_key = jax.random.fold_in(key, 23)
    coins = jax.random.randint(first_key, (N_BLK, 2 * REACH + 1), 0, 4)
    chosen = jnp.where(coins == 0, 1, 0).astype(jnp.int32)
    full_row = jax.random.randint(second_key, (), 0, N_BLK)
    row_index = lax.broadcasted_iota(jnp.int32, (N_BLK, 2 * REACH + 1), 0)
    col_index = lax.broadcasted_iota(jnp.int32, (N_BLK, 2 * REACH + 1), 1)
    chosen = jnp.where(row_index == full_row, 1, chosen)
    chosen = jnp.where(col_index == REACH, 1, chosen)
    return chosen.astype(jnp.int32)


def shard_levels(key, shape, pieces, least, high):
    level, own = 1.0, jax.random.fold_in(key, 6)
    for position, blocks in pieces:
        steps = jnp.exp(jax.random.uniform(jax.random.fold_in(own, position), (blocks,), jnp.float32, least / len(pieces), high / len(pieces)))
        level = level * jnp.repeat(steps, shape[position] // blocks).reshape([-1 if axis == position else 1 for axis in range(len(shape))])
    return level


def centred(own_key, dims, width, limit, shards=(), dtype=jnp.bfloat16):
    array = jax.random.normal(own_key, dims, jnp.float32) * width
    if len(shards) > 0:
        array = shard_levels(own_key, dims, shards, -0.22, 0.18) * array
    return jnp.clip(array, min=-limit, max=limit).astype(dtype)


def setup_inputs(seed: int = 0) -> dict:
    splits = jax.random.split(jax.random.key(seed), 7)
    image_emb = centred(splits[0], (IMAGES, D), D ** -0.5, 0.1875, ((0, 32),))
    text_emb = centred(splits[1], (IMAGES, D), D ** -0.5, 0.1875, ((0, 32),))
    positives = jax.vmap(lambda own: jax.random.permutation(own, ROWS))(jax.random.split(splits[2], (N_BLK * N_GRP))).reshape((N_BLK * N_GRP, ROWS)).astype(jnp.int32)
    pair_mask = draw_pair_mask(jax.random.fold_in(splits[6], 71), 0)
    log_scale = jnp.clip(jax.random.uniform(splits[4], (1,), jnp.float32, 1.5, 2.5), 1.5, 2.5)
    bias = jnp.clip(jax.random.uniform(splits[5], (1,), jnp.float32, -3.0, -1.0), -3.0, -1.0)
    return {"image_emb": image_emb, "text_emb": text_emb, "positives": positives, "pair_mask": pair_mask, "log_scale": log_scale, "bias": bias}


epsilon = 1e-06

def unit_rows(embedded):
    values = embedded.astype(jnp.float32)
    length = jnp.sqrt(lax.optimization_barrier(jnp.sum(values * values, axis=1, keepdims=True)) + epsilon)
    return (values / length, length)

def back_rows(normed, length, upstream):
    inward = lax.optimization_barrier(jnp.sum(normed * upstream, axis=1, keepdims=True))
    return (upstream - normed * inward) / length

def score_tile(image_side, text_side, labels, logit_scale, offset):
    similar = jnp.einsum('rd,cd->rc', image_side, text_side, preferred_element_type=jnp.float32)
    logits = logit_scale * similar + offset
    signed = labels * logits
    loss_sum = jnp.sum(jax.nn.softplus(-signed))
    slopes = (-labels * jax.nn.sigmoid(-signed) * logit_scale).astype(jnp.bfloat16)
    return (slopes, loss_sum)

def masked_tile(active_flag, image_side, text_side, labels, logit_scale, offset):

    def active(unused):
        return score_tile(image_side, text_side, labels, logit_scale, offset)

    def skipped(unused):
        return (jnp.zeros((image_side.shape[0], text_side.shape[0]), jnp.bfloat16), jnp.zeros((), jnp.float32))
    return lax.cond(active_flag > 0, active, skipped, 0)

def reference(image_emb, text_emb, positives, pair_mask, log_scale, bias):
    logit_scale = jnp.exp(log_scale[0])
    offset = bias[0]
    image_normed, image_len = unit_rows(image_emb)
    text_normed, text_len = unit_rows(text_emb)
    block_count = N_BLK * N_GRP
    image_blocks = image_normed.astype(jnp.bfloat16).reshape(block_count, ROWS, D)
    text_blocks = text_normed.astype(jnp.bfloat16).reshape(N_BLK, N_GRP, ROWS, D)
    columns = lax.broadcasted_iota(jnp.int32, (ROWS, ROWS), 1)
    image_total = jnp.zeros((block_count, ROWS, D), jnp.float32)
    text_total = jnp.zeros((N_BLK, N_GRP, ROWS, D), jnp.float32)
    loss_total = jnp.zeros((), jnp.float32)
    for distance in range(-REACH, REACH + 1):
        partner = jnp.roll(text_blocks, -distance, axis=0).reshape(block_count, ROWS, D)
        flags = jnp.broadcast_to(pair_mask[:, REACH + distance][:, None], (N_BLK, N_GRP)).reshape(block_count)

        def one_block(items, distance=distance):
            image_side, text_side, active_flag, matches = items
            if distance == 0:
                labels = jnp.where(matches[:, None] == columns, 1.0, -1.0).astype(jnp.float32)
            else:
                labels = -jnp.ones((ROWS, ROWS), jnp.float32)
            slopes, part_loss = masked_tile(active_flag, image_side, text_side, labels, logit_scale, offset)
            image_part = jnp.dot(slopes, text_side, preferred_element_type=jnp.float32)
            text_part = jnp.einsum('rc,rd->cd', slopes, image_side, preferred_element_type=jnp.float32)
            if distance != 0:
                text_part = lax.optimization_barrier(text_part.astype(jnp.bfloat16)).astype(jnp.float32)
            return (image_part, text_part, part_loss)
        image_part, text_part, parts = lax.map(one_block, (image_blocks, partner, flags, positives))
        image_total = image_total + image_part
        text_total = text_total + jnp.roll(text_part.reshape(N_BLK, N_GRP, ROWS, D), distance, axis=0)
        loss_total = loss_total + jnp.sum(parts)
    image_grad = back_rows(image_normed, image_len, image_total.reshape(IMAGES, D)).astype(jnp.bfloat16)
    text_grad = back_rows(text_normed, text_len, text_total.reshape(IMAGES, D)).astype(jnp.bfloat16)
    loss = (loss_total / IMAGES).reshape(1)
    return (image_grad, text_grad, loss)
```

```python
import functools

import jax
import jax.numpy as jnp
from jax import lax
from jax.experimental import pallas as pl
from jax.experimental.pallas import tpu as pltpu
from jax.sharding import PartitionSpec as P

epsilon = 1e-06


def passed_along(value, axis, steps):
    count = lax.axis_size(axis)
    pairs = [(source, (source + steps) % count) for source in range(count)]
    return lax.ppermute(value, axis, pairs)


def unit_rows(embedded):
    values = embedded.astype(jnp.float32)
    length = jnp.sqrt(jnp.sum(values * values, axis=1, keepdims=True) + epsilon)
    return (values / length, length)


def back_rows(normed, length, upstream):
    inward = jnp.sum(normed * upstream, axis=1, keepdims=True)
    return (upstream - normed * inward) / length


def score_tile(image_side, text_side, labels, logit_scale, offset):
    similar = jnp.einsum("rd,cd->rc", image_side, text_side, preferred_element_type=jnp.float32)
    logits = logit_scale * similar + offset
    signed = labels * logits
    loss_sum = jnp.sum(jax.nn.softplus(-signed))
    slopes = (-labels * jax.nn.sigmoid(-signed) * logit_scale).astype(jnp.bfloat16)
    return (slopes, loss_sum)


def masked_tile(active_flag, image_side, text_side, labels, logit_scale, offset):

    def active(unused):
        return score_tile(image_side, text_side, labels, logit_scale, offset)

    def skipped(unused):
        return (
            jnp.zeros((image_side.shape[0], text_side.shape[0]), jnp.bfloat16),
            jnp.zeros((), jnp.float32),
        )

    return lax.cond(active_flag > 0, active, skipped, 0)


def plain_body(image_emb, text_emb, positives, pair_mask, log_scale, bias):
    reach = (pair_mask.shape[1] - 1) // 2
    block_count = lax.axis_size("blk")
    myself = lax.axis_index("blk")
    logit_scale = jnp.exp(log_scale[0])
    offset = bias[0]
    row_count = image_emb.shape[0]
    image_normed, image_len = unit_rows(image_emb)
    text_normed, text_len = unit_rows(text_emb)
    image_half = image_normed.astype(jnp.bfloat16)
    text_half = text_normed.astype(jnp.bfloat16)
    columns = lax.broadcasted_iota(jnp.int32, (row_count, row_count), 1)
    own_labels = jnp.where(positives[0][:, None] == columns, 1.0, -1.0).astype(jnp.float32)
    apart_labels = -jnp.ones((row_count, row_count), jnp.float32)
    own_flags = lax.dynamic_index_in_dim(pair_mask, myself, 0, keepdims=False)
    fetched = {}
    for direction in (1, -1):
        moving = text_half
        for distance in range(1, reach + 1):
            moving = passed_along(moving, "blk", -direction)
            fetched[direction * distance] = moving
    slopes, loss_sum = masked_tile(
        own_flags[reach], image_half, text_half, own_labels, logit_scale, offset
    )
    image_total = jnp.dot(slopes, text_half, preferred_element_type=jnp.float32)
    text_total = jnp.einsum("rc,rd->cd", slopes, image_half, preferred_element_type=jnp.float32)
    for distance in range(-reach, reach + 1):
        if distance == 0:
            continue
        partner = fetched[distance]
        slopes, part_loss = masked_tile(
            own_flags[reach + distance], image_half, partner, apart_labels, logit_scale, offset
        )
        loss_sum = loss_sum + part_loss
        image_total = image_total + jnp.dot(slopes, partner, preferred_element_type=jnp.float32)
        partial_grad = jnp.einsum(
            "rc,rd->cd", slopes, image_half, preferred_element_type=jnp.float32
        ).astype(jnp.bfloat16)
        arrived = passed_along(partial_grad, "blk", distance)
        text_total = text_total + arrived.astype(jnp.float32)
    total_loss = lax.psum(loss_sum, ("blk", "grp"))
    image_count = row_count * block_count * lax.axis_size("grp")
    loss = (total_loss / image_count).reshape(1)
    image_grad = back_rows(image_normed, image_len, image_total).astype(jnp.bfloat16)
    text_grad = back_rows(text_normed, text_len, text_total).astype(jnp.bfloat16)
    return (image_grad, text_grad, loss)


MESH = pl.DeviceIdType.MESH
Y, INNER, OUTER = 0, 1, 2
OWN, OTHER = 0, 1


def grid_kernel(reach, parts, tiles, mask_ref, scale_ref, offset_ref, image_hbm, text_hbm, pos_hbm,
                image_out, text_out, loss_out,
                texts, images, pos_row, unit_texts, unit_images, labels, slopes, terms, sent, got,
                image_acc, image_sent, image_got, ready, loss_acc, blk_loss, grp_loss,
                load_sem, out_sem, send_sem, text_recv, image_recv, term_recv, back_recv,
                blk_send, blk_recv, grp_send, grp_recv):
    me = lax.axis_index("blk")
    grp = lax.axis_index("grp")
    count = lax.axis_size("blk")
    groups = lax.axis_size("grp")
    rows = images.shape[1]
    places = count // 2
    piece = rows // parts
    tall = rows // tiles
    per_tile = parts // tiles
    row, col = me // 2, me % 2
    top = row // 2
    role = row + top * (3 - 2 * row)
    toward = 1 - 2 * top
    aside = row * 2 + (1 - col)
    inner = (row + toward) * 2 + col
    outer = lax.rem((row - toward + 4), 4) * 2 + col
    targets = {Y: aside, INNER: inner, OUTER: outer}
    is_end, is_mid = role == 0, role == 1

    def place_row(p):
        return p + top * (3 - 2 * p)

    def cut(c):
        return pl.ds(pl.multiple_of(c * piece, piece), piece)

    def at(which, c):
        return pl.ds(pl.multiple_of(which * rows + c * piece, piece), piece)

    def tile_at(which, c):
        return pl.ds(pl.multiple_of(which * rows + c * tall, tall), tall)

    def send(way, slot, c, source, target, recv):
        return pltpu.make_async_remote_copy(
            src_ref=source, dst_ref=target, send_sem=send_sem.at[way, slot, c], recv_sem=recv,
            device_id=(targets[way], grp), device_id_type=MESH)

    def text_copy(way, slot, which, c):
        return send(way, slot, c, texts.at[at(which, c)], texts.at[at(which, c)], text_recv.at[which, c])

    def image_copy(c):
        return send(Y, 0, c, images.at[OWN, cut(c)], images.at[OTHER, cut(c)], image_recv.at[c])

    def back_copy(c):
        return send(Y, 1, c, image_sent.at[cut(c)], image_got.at[cut(c)], back_recv.at[c])

    def term_copy(way, slot, which, side, c):
        return send(way, slot, c, sent.at[at(which, c)], got.at[side, at(which, c)], term_recv.at[side, which, c])

    def term_arrived(side, which, c):
        term_copy(INNER, 0, which, side, c).wait_recv()

    own_row = place_row(role)
    loads = [
        pltpu.make_async_copy(text_hbm, texts.at[pl.ds(pl.multiple_of(own_row * rows, rows), rows)], load_sem.at[0]),
        pltpu.make_async_copy(image_hbm, images.at[OWN], load_sem.at[1]),
        pltpu.make_async_copy(pos_hbm, pos_row, load_sem.at[2]),
    ]
    for load in loads:
        load.start()
    barrier = pltpu.get_barrier_semaphore()

    @pl.loop(1, count)
    def _(d):
        pl.semaphore_signal(barrier, inc=1, device_id=(lax.rem(me + d, count), grp), device_id_type=MESH)

    @pl.loop(1, groups)
    def _(d):
        pl.semaphore_signal(barrier, inc=1, device_id=(me, lax.rem(grp + d, groups)), device_id_type=MESH)

    pl.semaphore_wait(barrier, count + groups - 2)

    def blk_share(d):
        target = lax.rem(me + d, count)
        return pltpu.make_async_remote_copy(
            src_ref=blk_loss.at[me], dst_ref=blk_loss.at[me], send_sem=blk_send.at[d],
            recv_sem=blk_recv.at[me], device_id=(target, grp), device_id_type=MESH)

    def blk_arrival(d):
        source = lax.rem(me + d, count)
        return pltpu.make_async_remote_copy(
            src_ref=blk_loss.at[source], dst_ref=blk_loss.at[source], send_sem=blk_send.at[d],
            recv_sem=blk_recv.at[source], device_id=(source, grp), device_id_type=MESH)

    def grp_share(d):
        target = lax.rem(grp + d, groups)
        return pltpu.make_async_remote_copy(
            src_ref=grp_loss.at[grp], dst_ref=grp_loss.at[grp], send_sem=grp_send.at[d],
            recv_sem=grp_recv.at[grp], device_id=(me, target), device_id_type=MESH)

    def grp_arrival(d):
        source = lax.rem(grp + d, groups)
        return pltpu.make_async_remote_copy(
            src_ref=grp_loss.at[source], dst_ref=grp_loss.at[source], send_sem=grp_send.at[d],
            recv_sem=grp_recv.at[source], device_id=(me, source), device_id_type=MESH)

    loads[0].wait()

    @pl.loop(0, parts)
    def _(c):
        text_copy(INNER, 0, own_row, c).start()

        @pl.when(is_mid)
        def _():
            text_copy(OUTER, 0, own_row, c).start()

    loads[1].wait()

    @pl.loop(0, parts)
    def _(c):
        image_copy(c).start()

    scale = jnp.exp(jnp.full((1, 1), scale_ref[0], jnp.float32))
    offset = jnp.full((1, 1), offset_ref[0], jnp.float32)

    def unit(values):
        length = jnp.sqrt(jnp.sum(values * values, axis=1, keepdims=True) + epsilon)
        return values / length, length

    loss_acc[...] = jnp.zeros_like(loss_acc)
    loads[2].wait()

    @pl.loop(0, tiles)
    def _(c):
        band = pl.ds(pl.multiple_of(c * tall, tall), tall)
        unit_images[band, :] = unit(images[OWN, band, :].astype(jnp.float32))[0].astype(jnp.bfloat16)
        hit = pos_row[...] == lax.broadcasted_iota(jnp.int32, (tall, rows), 0) + c * tall
        labels[1 + c] = jnp.transpose(jnp.where(hit, -1.0, 1.0))

    labels[0] = jnp.full(labels.shape[1:], 1.0, jnp.float32)

    @pl.loop(0, parts)
    def _(c):
        @pl.when(is_mid)
        def _():
            text_copy(Y, 0, place_row(0), c).wait_recv()
            text_copy(INNER, 1, place_row(0), c).start()
            text_copy(Y, 0, place_row(2), c).wait_recv()
            text_copy(OUTER, 1, place_row(2), c).start()

        image_copy(c).wait_recv()
        unit_images[at(1, c), :] = unit(images[OTHER, cut(c), :].astype(jnp.float32))[0].astype(jnp.bfloat16)

    def flag_of(other, which):
        image = row * 2 + col + other * (1 - 2 * col)
        text = which * 2 + col
        apart = lax.rem(text - image + reach + count, count)
        inside = 1 - apart // (2 * reach + 1)
        return (mask_ref[image, apart * inside] * inside).astype(jnp.float32)

    def item(p, which, c):
        text = unit(texts[tile_at(which, c), :].astype(jnp.float32))[0].astype(jnp.bfloat16)
        unit_texts[tile_at(which, c), :] = text
        own = 1 // (1 + (p - role) * (p - role))
        term = None
        for other in (OWN, OTHER):
            flag = flag_of(other, which)
            side = unit_images[other * rows:(other + 1) * rows, :]
            similar = lax.dot_general(side, text, (((1,), (1,)), ((), ())), preferred_element_type=jnp.float32)
            logits = scale * similar + offset
            factor = scale * flag
            if other == OWN:
                label = labels[(1 + c) * own]
                logits = logits * label
                factor = factor * label
            grown = jnp.exp(logits)
            lifted = 1.0 + grown
            slope = (grown / lifted * factor).astype(jnp.bfloat16)
            slopes[other, :, tile_at(which, c)] = slope
            loss_acc[...] += flag * jnp.sum(jnp.log(lifted), axis=0, keepdims=True)
            part = lax.dot_general(slope, side, (((0,), (0,)), ((), ())), preferred_element_type=jnp.float32)
            term = part if term is None else term + part
        terms[tile_at(which, c), :] = term
        sent[tile_at(which, c), :] = term.astype(jnp.bfloat16)

    def relay(way, slot, side, p, c):
        which = place_row(p)
        term_arrived(side, which, c)
        total = terms[at(which, c), :] + got[side, at(which, c), :].astype(jnp.float32)
        sent[at(which, c), :] = total.astype(jnp.bfloat16)
        term_copy(way, slot, which, 1, c).start()

    steps = 4 * tiles

    @pl.loop(0, steps)
    def _(s):
        third = s // tiles
        first, last = (tiles - third) // tiles, third // tiles
        between, odd = 1 - first - last, (s + 1) % 2
        p = (first * (1 + role) + last * (3 - 2 * role)
             + between * ((1 - odd) * (2 - 2 * role) + odd * 3 * role))
        c = first * s + last * (s - 3 * tiles) + between * ((s + 1) // 2 - 2)
        which = place_row(p)

        @pl.when((1 - role) * p > 0)
        def _():
            @pl.loop(0, per_tile)
            def _(k):
                text_copy(Y, 0, which, c * per_tile + k).wait_recv()

        @pl.when(role * (p // 3) == 1)
        def _():
            @pl.loop(0, per_tile)
            def _(k):
                text_copy(Y, 0, which, c * per_tile + k).wait_recv()
                text_copy(OUTER, 2, which, c * per_tile + k).start()

        item(p, which, c)

        @pl.when((1 - role) * p * (p // 3 + (tiles - c) // 2) > 0)
        def _():
            @pl.loop(0, per_tile)
            def _(k):
                term_copy(INNER, p, which, 0, c * per_tile + k).start()

        @pl.when(role * (s // 7) * (1 - s // 11) == 1)
        def _():
            relay(INNER, 2, 0, 2, s - 7)

    @pl.when(is_end)
    def _():
        @pl.loop(0, 2 * per_tile)
        def _(k):
            p = 2 - k // per_tile
            term_copy(INNER, p, place_row(p), 0, parts - per_tile + k % per_tile).start()

    blk_loss[me] = jnp.full(blk_loss.shape[1:], jnp.sum(loss_acc[...]), jnp.float32)

    @pl.loop(1, count)
    def _(d):
        blk_share(d).start()

    @pl.loop(0, parts)
    def _(c):
        @pl.when(is_mid)
        def _():
            relay(INNER, 3, 0, 3, c)

        whole = jnp.dot(slopes[OTHER, cut(c), :], unit_texts[...], preferred_element_type=jnp.float32)
        image_sent[cut(c), :] = whole.astype(jnp.bfloat16)
        back_copy(c).start()
        image_acc[cut(c), :] = jnp.dot(
            slopes[OWN, cut(c), :], unit_texts[...], preferred_element_type=jnp.float32)

        @pl.when(role * c > 0)
        def _():
            relay(OUTER, 3, 1, 0, c - 1)

    @pl.when(is_mid)
    def _():
        relay(OUTER, 3, 1, 0, parts - 1)

        @pl.loop(parts - per_tile, parts)
        def _(c):
            relay(INNER, 2, 0, 2, c)

    @pl.loop(1, count)
    def _(d):
        blk_arrival(d).wait_recv()

    grp_loss[grp] = jnp.sum(blk_loss[...], axis=0)

    @pl.loop(1, groups)
    def _(d):
        grp_share(d).start()

    def put_out(side, result, c):
        return pltpu.make_async_copy(ready.at[side, cut(c)], result.at[cut(c)], out_sem.at[side, c])

    def finish(side, source, upstream, result, c):
        normed, length = unit(source.astype(jnp.float32))
        ready[side, cut(c), :] = back_rows(normed, length, upstream).astype(ready.dtype)
        put_out(side, result, c).start()

    @pl.loop(0, parts)
    def _(c):
        term_arrived(1, own_row, c)

        @pl.when(is_mid)
        def _():
            term_arrived(0, own_row, c)
            terms[at(own_row, c), :] += got[0, at(own_row, c), :].astype(jnp.float32)

        total = terms[at(own_row, c), :] + got[1, at(own_row, c), :].astype(jnp.float32)
        finish(1, texts[at(own_row, c), :], total, text_out, c)
        back_copy(c).wait_recv()
        total = image_acc[cut(c), :] + image_got[cut(c), :].astype(jnp.float32)
        finish(0, images[OWN, cut(c), :], total, image_out, c)

    @pl.loop(1, groups)
    def _(d):
        grp_arrival(d).wait_recv()

    total = jnp.sum(grp_loss[...], axis=0)
    loss_out[0] = jnp.sum(total[0:1, 0:1]) / (rows * count * groups)

    @pl.loop(1, count)
    def _(d):
        blk_share(d).wait_send()

    @pl.loop(1, groups)
    def _(d):
        grp_share(d).wait_send()

    @pl.loop(0, parts)
    def _(c):
        put_out(0, image_out, c).wait()
        put_out(1, text_out, c).wait()
        for slot in range(2):
            text_copy(Y, slot, own_row, c).wait_send()
        for slot in range(4):
            text_copy(INNER, slot, own_row, c).wait_send()

        @pl.when(is_mid)
        def _():
            for slot in range(4):
                text_copy(OUTER, slot, own_row, c).wait_send()


def body(image_emb, text_emb, positives, pair_mask, log_scale, bias):
    reach = (pair_mask.shape[1] - 1) // 2
    block_count = lax.axis_size("blk")
    row_count, width = image_emb.shape
    if block_count != 2 * (reach + 1) or reach != 3 or row_count % (3 * 128) != 0:
        return plain_body(image_emb, text_emb, positives, pair_mask, log_scale, bias)
    parts, tiles = 6, 3
    places = block_count // 2
    groups = lax.axis_size("grp")
    smem = pl.BlockSpec(memory_space=pltpu.SMEM)
    anywhere = pl.BlockSpec(memory_space=pl.ANY)
    column = places * row_count
    return pl.pallas_call(
        functools.partial(grid_kernel, reach, parts, tiles),
        out_shape=(
            jax.ShapeDtypeStruct(image_emb.shape, image_emb.dtype),
            jax.ShapeDtypeStruct(text_emb.shape, text_emb.dtype),
            jax.ShapeDtypeStruct((1,), jnp.float32),
        ),
        in_specs=[smem] * 3 + [anywhere] * 3,
        out_specs=(anywhere, anywhere, smem),
        scratch_shapes=[
            pltpu.VMEM((column, width), jnp.bfloat16),
            pltpu.VMEM((2, row_count, width), jnp.bfloat16),
            pltpu.VMEM((1, row_count), jnp.int32),
            pltpu.VMEM((column, width), jnp.bfloat16),
            pltpu.VMEM((2 * row_count, width), jnp.bfloat16),
            pltpu.VMEM((1 + tiles, row_count, row_count // tiles), jnp.float32),
            pltpu.VMEM((2, row_count, column), jnp.bfloat16),
            pltpu.VMEM((column, width), jnp.float32),
            pltpu.VMEM((column, width), jnp.bfloat16),
            pltpu.VMEM((2, column, width), jnp.bfloat16),
            pltpu.VMEM((row_count, width), jnp.float32),
            pltpu.VMEM((row_count, width), jnp.bfloat16),
            pltpu.VMEM((row_count, width), jnp.bfloat16),
            pltpu.VMEM((2, row_count, width), jnp.bfloat16),
            pltpu.VMEM((1, row_count // tiles), jnp.float32),
            pltpu.VMEM((block_count, 8, 128), jnp.float32),
            pltpu.VMEM((groups, 8, 128), jnp.float32),
            pltpu.SemaphoreType.DMA((3,)),
            pltpu.SemaphoreType.DMA((2, parts)),
            pltpu.SemaphoreType.DMA((3, 4, parts)),
            pltpu.SemaphoreType.DMA((places, parts)),
            pltpu.SemaphoreType.DMA((parts,)),
            pltpu.SemaphoreType.DMA((2, places, parts)),
            pltpu.SemaphoreType.DMA((parts,)),
            pltpu.SemaphoreType.DMA((block_count,)),
            pltpu.SemaphoreType.DMA((block_count,)),
            pltpu.SemaphoreType.DMA((groups,)),
            pltpu.SemaphoreType.DMA((groups,)),
        ],
        compiler_params=pltpu.CompilerParams(
            collective_id=0, has_side_effects=True, vmem_limit_bytes=67043328
        ),
    )(pair_mask, log_scale, bias, image_emb, text_emb, positives)


def solution(mesh):
    return jax.shard_map(
        body,
        mesh=mesh,
        in_specs=(
            P(("blk", "grp"), None),
            P(("blk", "grp"), None),
            P(("blk", "grp"), None),
            P(),
            P(),
            P(),
        ),
        out_specs=(P(("blk", "grp"), None), P(("blk", "grp"), None), P()),
        check_vma=False,
    )
```

```python
import functools

import jax
import jax.numpy as jnp
from jax import lax
from jax.experimental import pallas as pl
from jax.experimental.pallas import tpu as pltpu
from jax.sharding import PartitionSpec as P

epsilon = 1e-06


def passed_along(value, axis, steps):
    count = lax.axis_size(axis)
    pairs = [(source, (source + steps) % count) for source in range(count)]
    return lax.ppermute(value, axis, pairs)


def unit_rows(embedded):
    values = embedded.astype(jnp.float32)
    length = jnp.sqrt(jnp.sum(values * values, axis=1, keepdims=True) + epsilon)
    return (values / length, length)


def back_rows(normed, length, upstream):
    inward = jnp.sum(normed * upstream, axis=1, keepdims=True)
    return (upstream - normed * inward) / length


def score_tile(image_side, text_side, labels, logit_scale, offset):
    similar = jnp.einsum("rd,cd->rc", image_side, text_side, preferred_element_type=jnp.float32)
    logits = logit_scale * similar + offset
    signed = labels * logits
    loss_sum = jnp.sum(jax.nn.softplus(-signed))
    slopes = (-labels * jax.nn.sigmoid(-signed) * logit_scale).astype(jnp.bfloat16)
    return (slopes, loss_sum)


def masked_tile(active_flag, image_side, text_side, labels, logit_scale, offset):

    def active(unused):
        return score_tile(image_side, text_side, labels, logit_scale, offset)

    def skipped(unused):
        return (
            jnp.zeros((image_side.shape[0], text_side.shape[0]), jnp.bfloat16),
            jnp.zeros((), jnp.float32),
        )

    return lax.cond(active_flag > 0, active, skipped, 0)


def plain_body(image_emb, text_emb, positives, pair_mask, log_scale, bias):
    reach = (pair_mask.shape[1] - 1) // 2
    block_count = lax.axis_size("blk")
    myself = lax.axis_index("blk")
    logit_scale = jnp.exp(log_scale[0])
    offset = bias[0]
    row_count = image_emb.shape[0]
    image_normed, image_len = unit_rows(image_emb)
    text_normed, text_len = unit_rows(text_emb)
    image_half = image_normed.astype(jnp.bfloat16)
    text_half = text_normed.astype(jnp.bfloat16)
    columns = lax.broadcasted_iota(jnp.int32, (row_count, row_count), 1)
    own_labels = jnp.where(positives[0][:, None] == columns, 1.0, -1.0).astype(jnp.float32)
    apart_labels = -jnp.ones((row_count, row_count), jnp.float32)
    own_flags = lax.dynamic_index_in_dim(pair_mask, myself, 0, keepdims=False)
    fetched = {}
    for direction in (1, -1):
        moving = text_half
        for distance in range(1, reach + 1):
            moving = passed_along(moving, "blk", -direction)
            fetched[direction * distance] = moving
    slopes, loss_sum = masked_tile(
        own_flags[reach], image_half, text_half, own_labels, logit_scale, offset
    )
    image_total = jnp.dot(slopes, text_half, preferred_element_type=jnp.float32)
    text_total = jnp.einsum("rc,rd->cd", slopes, image_half, preferred_element_type=jnp.float32)
    for distance in range(-reach, reach + 1):
        if distance == 0:
            continue
        partner = fetched[distance]
        slopes, part_loss = masked_tile(
            own_flags[reach + distance], image_half, partner, apart_labels, logit_scale, offset
        )
        loss_sum = loss_sum + part_loss
        image_total = image_total + jnp.dot(slopes, partner, preferred_element_type=jnp.float32)
        partial_grad = jnp.einsum(
            "rc,rd->cd", slopes, image_half, preferred_element_type=jnp.float32
        ).astype(jnp.bfloat16)
        arrived = passed_along(partial_grad, "blk", distance)
        text_total = text_total + arrived.astype(jnp.float32)
    total_loss = lax.psum(loss_sum, ("blk", "grp"))
    image_count = row_count * block_count * lax.axis_size("grp")
    loss = (total_loss / image_count).reshape(1)
    image_grad = back_rows(image_normed, image_len, image_total).astype(jnp.bfloat16)
    text_grad = back_rows(text_normed, text_len, text_total).astype(jnp.bfloat16)
    return (image_grad, text_grad, loss)


MESH = pl.DeviceIdType.MESH
Y, INNER, OUTER = 0, 1, 2
OWN, OTHER = 0, 1


def grid_kernel(reach, parts, tiles, mask_hbm, scale_hbm, offset_hbm, image_hbm, text_hbm, pos_hbm,
                image_out, text_out, loss_out,
                mask_ref, scale_ref, offset_ref, loss_ref,
                texts, images, pos_row, unit_texts, unit_images, labels, slopes, terms, sent, got,
                image_acc, image_sent, image_got, loss_acc, line_loss, plane_loss,
                load_sem, send_sem, text_recv, image_recv, term_recv, back_recv,
                line_send, line_recv, plane_send, plane_recv):
    me = lax.axis_index("blk")
    grp = lax.axis_index("grp")
    count = lax.axis_size("blk")
    groups = lax.axis_size("grp")
    rows = images.shape[1]
    places = count // 2
    piece = rows // parts
    tall = rows // tiles
    per_tile = parts // tiles
    row, col = me // 2, me % 2
    top = row // 2
    role = row + top * (3 - 2 * row)
    toward = 1 - 2 * top
    aside = row * 2 + (1 - col)
    inner = (row + toward) * 2 + col
    outer = lax.rem((row - toward + 4), 4) * 2 + col
    targets = {Y: aside, INNER: inner, OUTER: outer}
    is_end, is_mid = role == 0, role == 1

    def place_row(p):
        return p + top * (3 - 2 * p)

    def cut(c):
        return pl.ds(pl.multiple_of(c * piece, piece), piece)

    def at(which, c):
        return pl.ds(pl.multiple_of(which * rows + c * piece, piece), piece)

    def tile_at(which, c):
        return pl.ds(pl.multiple_of(which * rows + c * tall, tall), tall)

    def send(way, slot, source, target, recv):
        return pltpu.make_async_remote_copy(
            src_ref=source, dst_ref=target, send_sem=send_sem.at[way, slot], recv_sem=recv,
            device_id=(targets[way], grp), device_id_type=MESH)

    def text_copy(way, slot, which, c):
        return send(way, slot, texts.at[at(which, c)], texts.at[at(which, c)], text_recv.at[which, c])

    def image_copy(c):
        return send(Y, 0, images.at[OWN, cut(c)], images.at[OTHER, cut(c)], image_recv.at[c])

    def back_copy(c):
        return send(Y, 1, image_sent.at[cut(c)], image_got.at[cut(c)], back_recv.at[c])

    def term_copy(way, slot, which, kind, c):
        return send(way, slot, sent.at[at(which, c)], got.at[kind, cut(c)], term_recv.at[kind, c])

    def term_arrived(kind, c):
        term_copy(INNER, 0, 0, kind, c).wait_recv()

    def all_sent(way, slot):
        block = texts.at[pl.ds(0, rows)]
        send(way, slot, block, block, text_recv.at[0, 0]).wait_send()

    own_row = place_row(role)
    loads = [
        pltpu.make_async_copy(source, target, load_sem.at[i])
        for i, (source, target) in enumerate((
            (text_hbm, texts.at[pl.ds(pl.multiple_of(own_row * rows, rows), rows)]),
            (image_hbm, images.at[OWN]), (pos_hbm, pos_row),
            (mask_hbm, mask_ref), (scale_hbm, scale_ref), (offset_hbm, offset_ref)))
    ]
    for load in loads:
        load.start()
    barrier = pltpu.get_barrier_semaphore()
    plane = 2 * groups
    spot = col * groups + grp

    def in_plane(d):
        other = lax.rem(spot + d, plane)
        return other, (row * 2 + other // groups, lax.rem(other, groups))

    pl.semaphore_signal(barrier, inc=1, device_id=(inner, grp), device_id_type=MESH)

    @pl.when(is_mid)
    def _():
        pl.semaphore_signal(barrier, inc=1, device_id=(outer, grp), device_id_type=MESH)

    @pl.loop(1, plane)
    def _(d):
        pl.semaphore_signal(barrier, inc=1, device_id=in_plane(d)[1], device_id_type=MESH)

    pl.semaphore_wait(barrier, plane + role)

    def line_share(d):
        target = lax.rem(row + d, places)
        return pltpu.make_async_remote_copy(
            src_ref=line_loss.at[row], dst_ref=line_loss.at[row], send_sem=line_send.at[0],
            recv_sem=line_recv.at[row], device_id=(target * 2 + col, grp), device_id_type=MESH)

    def line_arrival(d):
        source = lax.rem(row + d, places)
        return pltpu.make_async_remote_copy(
            src_ref=line_loss.at[source], dst_ref=line_loss.at[source], send_sem=line_send.at[0],
            recv_sem=line_recv.at[source], device_id=(source * 2 + col, grp), device_id_type=MESH)

    def plane_share(d):
        return pltpu.make_async_remote_copy(
            src_ref=plane_loss.at[spot], dst_ref=plane_loss.at[spot], send_sem=plane_send.at[0],
            recv_sem=plane_recv.at[spot], device_id=in_plane(d)[1], device_id_type=MESH)

    def plane_arrival(d):
        other, device = in_plane(d)
        return pltpu.make_async_remote_copy(
            src_ref=plane_loss.at[other], dst_ref=plane_loss.at[other], send_sem=plane_send.at[0],
            recv_sem=plane_recv.at[other], device_id=device, device_id_type=MESH)

    loads[0].wait()

    @pl.loop(0, parts)
    def _(c):
        text_copy(INNER, 0, own_row, c).start()

        @pl.when(is_mid)
        def _():
            text_copy(OUTER, 0, own_row, c).start()

    loads[1].wait()

    @pl.loop(0, parts)
    def _(c):
        image_copy(c).start()

    for load in loads[2:]:
        load.wait()

    scale = jnp.exp(jnp.full((1, 1), scale_ref[0], jnp.float32))
    offset = jnp.full((1, 1), offset_ref[0], jnp.float32)

    def unit(values):
        length = jnp.sqrt(jnp.sum(values * values, axis=1, keepdims=True) + epsilon)
        return values / length, length

    loss_acc[...] = jnp.zeros_like(loss_acc)

    @pl.loop(0, tiles)
    def _(c):
        band = pl.ds(pl.multiple_of(c * tall, tall), tall)
        unit_images[band, :] = unit(images[OWN, band, :].astype(jnp.float32))[0].astype(jnp.bfloat16)
        hit = pos_row[...] == lax.broadcasted_iota(jnp.int32, (tall, rows), 0) + c * tall
        labels[1 + c] = jnp.transpose(jnp.where(hit, -1.0, 1.0))

    labels[0] = jnp.full(labels.shape[1:], 1.0, jnp.float32)

    @pl.loop(0, parts)
    def _(c):
        @pl.when(is_mid)
        def _():
            text_copy(Y, 0, place_row(0), c).wait_recv()
            text_copy(INNER, 1, place_row(0), c).start()
            text_copy(Y, 0, place_row(2), c).wait_recv()
            text_copy(OUTER, 1, place_row(2), c).start()

        image_copy(c).wait_recv()
        unit_images[at(1, c), :] = unit(images[OTHER, cut(c), :].astype(jnp.float32))[0].astype(jnp.bfloat16)

    def flag_of(other, which):
        image = row * 2 + col + other * (1 - 2 * col)
        text = which * 2 + col
        apart = lax.rem(text - image + reach + count, count)
        inside = 1 - apart // (2 * reach + 1)
        return (mask_ref[image, apart * inside] * inside).astype(jnp.float32)

    def item(p, which, c):
        text = unit(texts[tile_at(which, c), :].astype(jnp.float32))[0].astype(jnp.bfloat16)
        unit_texts[tile_at(which, c), :] = text
        own = 1 // (1 + (p - role) * (p - role))
        term = None
        for other in (OWN, OTHER):
            flag = flag_of(other, which)
            side = unit_images[other * rows:(other + 1) * rows, :]
            similar = lax.dot_general(side, text, (((1,), (1,)), ((), ())), preferred_element_type=jnp.float32)
            logits = scale * similar + offset
            factor = scale * flag
            if other == OWN:
                label = labels[(1 + c) * own]
                logits = logits * label
                factor = factor * label
            grown = jnp.exp(logits)
            lifted = 1.0 + grown
            slope = (grown / lifted * factor).astype(jnp.bfloat16)
            slopes[other, :, tile_at(which, c)] = slope
            loss_acc[...] += flag * jnp.sum(jnp.log(lifted), axis=0, keepdims=True)
            part = lax.dot_general(slope, side, (((0,), (0,)), ((), ())), preferred_element_type=jnp.float32)
            term = part if term is None else term + part
        terms[tile_at(which, c), :] = term
        sent[tile_at(which, c), :] = term.astype(jnp.bfloat16)

    def relay(way, slot, kind, p, onward, c):
        which = place_row(p)
        term_arrived(kind, c)
        total = terms[at(which, c), :] + got[kind, cut(c), :].astype(jnp.float32)
        sent[at(which, c), :] = total.astype(jnp.bfloat16)
        term_copy(way, slot, which, onward, c).start()

    steps = 4 * tiles

    @pl.loop(0, steps)
    def _(s):
        third = s // tiles
        first, last = (tiles - third) // tiles, third // tiles
        between, odd = 1 - first - last, (s + 1) % 2
        p = (first * (1 + role) + last * (3 - 2 * role)
             + between * ((1 - odd) * (2 - 2 * role) + odd * 3 * role))
        c = first * s + last * (s - 3 * tiles) + between * ((s + 1) // 2 - 2)
        which = place_row(p)

        @pl.when((1 - role) * p > 0)
        def _():
            @pl.loop(0, per_tile)
            def _(k):
                text_copy(Y, 0, which, c * per_tile + k).wait_recv()

        @pl.when(role * (p // 3) == 1)
        def _():
            @pl.loop(0, per_tile)
            def _(k):
                text_copy(Y, 0, which, c * per_tile + k).wait_recv()
                text_copy(OUTER, 2, which, c * per_tile + k).start()

        item(p, which, c)

        @pl.when(s == steps - 1)
        def _():
            line_loss[row] = jnp.full(line_loss.shape[1:], jnp.sum(loss_acc[...]), jnp.float32)

            @pl.loop(1, places)
            def _(d):
                line_share(d).start()

        @pl.when((1 - role) * p * (p // 3 + (tiles - c) // 2) > 0)
        def _():
            @pl.loop(0, per_tile)
            def _(k):
                term_copy(INNER, p, which, p - 1, c * per_tile + k).start()

        @pl.when(role * (s // 7) * (1 - s // 11) == 1)
        def _():
            relay(INNER, 2, 1, 2, 3, s - 7)

    @pl.when(is_end)
    def _():
        @pl.loop(0, 2 * per_tile)
        def _(k):
            p = 2 - k // per_tile
            term_copy(INNER, p, place_row(p), p - 1, parts - per_tile + k % per_tile).start()

    @pl.loop(0, parts)
    def _(c):
        @pl.when(is_mid)
        def _():
            relay(INNER, 3, 2, 3, 4, c)

        whole = jnp.dot(slopes[OTHER, cut(c), :], unit_texts[...], preferred_element_type=jnp.float32)
        image_sent[cut(c), :] = whole.astype(jnp.bfloat16)
        back_copy(c).start()
        image_acc[cut(c), :] = jnp.dot(
            slopes[OWN, cut(c), :], unit_texts[...], preferred_element_type=jnp.float32)

        @pl.when(role * c > 0)
        def _():
            relay(OUTER, 3, 4, 0, 3, c - 1)

        @pl.when(c == parts - 1)
        def _():
            @pl.loop(1, places)
            def _(d):
                line_arrival(d).wait_recv()

            plane_loss[spot] = jnp.sum(line_loss[...], axis=0)

            @pl.loop(1, plane)
            def _(d):
                plane_share(d).start()

    @pl.when(is_mid)
    def _():
        relay(OUTER, 3, 4, 0, 3, parts - 1)

        @pl.loop(parts - per_tile, parts)
        def _(c):
            relay(INNER, 2, 1, 2, 3, c)

    def put_loss():
        return pltpu.make_async_copy(loss_ref, loss_out, load_sem.at[0])

    def finish(source, upstream, result, c):
        normed, length = unit(source.astype(jnp.float32))
        result[cut(c), :] = back_rows(normed, length, upstream).astype(result.dtype)

    @pl.loop(0, parts)
    def _(c):
        @pl.when(c == parts // 2)
        def _():
            @pl.loop(1, plane)
            def _(d):
                plane_arrival(d).wait_recv()

            total = jnp.sum(plane_loss[...], axis=0)
            loss_ref[0] = jnp.sum(total[0:1, 0:1]) / (rows * count * groups)
            put_loss().start()

        @pl.when(is_mid)
        def _():
            term_arrived(0, c)
            terms[at(own_row, c), :] += got[0, cut(c), :].astype(jnp.float32)

        term_arrived(3, c)
        total = terms[at(own_row, c), :] + got[3, cut(c), :].astype(jnp.float32)
        finish(texts[at(own_row, c), :], total, text_out, c)
        back_copy(c).wait_recv()
        total = image_acc[cut(c), :] + image_got[cut(c), :].astype(jnp.float32)
        finish(images[OWN, cut(c), :], total, image_out, c)

    put_loss().wait()
    lines = line_loss.at[pl.ds(0, places - 1)]
    pltpu.make_async_remote_copy(
        src_ref=lines, dst_ref=lines, send_sem=line_send.at[0], recv_sem=line_recv.at[0],
        device_id=(inner, grp), device_id_type=MESH).wait_send()
    planes = plane_loss.at[pl.ds(0, plane - 1)]
    pltpu.make_async_remote_copy(
        src_ref=planes, dst_ref=planes, send_sem=plane_send.at[0], recv_sem=plane_recv.at[0],
        device_id=(inner, grp), device_id_type=MESH).wait_send()
    for slot in range(2):
        all_sent(Y, slot)
    for slot in range(4):
        all_sent(INNER, slot)

    @pl.when(is_mid)
    def _():
        for slot in range(4):
            all_sent(OUTER, slot)


def store_kernel(pieces, image_ref, text_ref, image_out, text_out, sem):
    height = image_ref.shape[0] // pieces
    copies = [
        pltpu.make_async_copy(source.at[pl.ds(c * height, height)], result.at[pl.ds(c * height, height)], sem.at[i, c])
        for i, (source, result) in enumerate(((image_ref, image_out), (text_ref, text_out)))
        for c in range(pieces)
    ]
    for copy in copies:
        copy.start()
    for copy in copies:
        copy.wait()


def body(image_emb, text_emb, positives, pair_mask, log_scale, bias):
    reach = (pair_mask.shape[1] - 1) // 2
    block_count = lax.axis_size("blk")
    row_count, width = image_emb.shape
    if block_count != 2 * (reach + 1) or reach != 3 or row_count % (3 * 128) != 0:
        return plain_body(image_emb, text_emb, positives, pair_mask, log_scale, bias)
    parts, tiles = 6, 3
    places = block_count // 2
    groups = lax.axis_size("grp")
    vmem = pl.BlockSpec(memory_space=pltpu.VMEM)
    anywhere = pl.BlockSpec(memory_space=pl.ANY)
    column = places * row_count
    grant = 67043328 - 2 * image_emb.size * image_emb.dtype.itemsize
    image_grad, text_grad, loss = pl.pallas_call(
        functools.partial(grid_kernel, reach, parts, tiles),
        out_shape=(
            pltpu.VMEM(image_emb.shape, image_emb.dtype),
            pltpu.VMEM(text_emb.shape, text_emb.dtype),
            jax.ShapeDtypeStruct((1,), jnp.float32),
        ),
        in_specs=[pl.BlockSpec(memory_space=pltpu.HBM)] * 6,
        out_specs=(vmem, vmem, anywhere),
        scratch_shapes=[
            pltpu.SMEM(pair_mask.shape, jnp.int32),
            pltpu.SMEM((1,), jnp.float32),
            pltpu.SMEM((1,), jnp.float32),
            pltpu.SMEM((1,), jnp.float32),
            pltpu.VMEM((column, width), jnp.bfloat16),
            pltpu.VMEM((2, row_count, width), jnp.bfloat16),
            pltpu.VMEM((1, row_count), jnp.int32),
            pltpu.VMEM((column, width), jnp.bfloat16),
            pltpu.VMEM((2 * row_count, width), jnp.bfloat16),
            pltpu.VMEM((1 + tiles, row_count, row_count // tiles), jnp.float32),
            pltpu.VMEM((2, row_count, column), jnp.bfloat16),
            pltpu.VMEM((column, width), jnp.float32),
            pltpu.VMEM((column, width), jnp.bfloat16),
            pltpu.VMEM((5, row_count, width), jnp.bfloat16),
            pltpu.VMEM((row_count, width), jnp.float32),
            pltpu.VMEM((row_count, width), jnp.bfloat16),
            pltpu.VMEM((row_count, width), jnp.bfloat16),
            pltpu.VMEM((1, row_count // tiles), jnp.float32),
            pltpu.VMEM((places, 8, 128), jnp.float32),
            pltpu.VMEM((2 * groups, 8, 128), jnp.float32),
            pltpu.SemaphoreType.DMA((6,)),
            pltpu.SemaphoreType.DMA((3, 4)),
            pltpu.SemaphoreType.DMA((places, parts)),
            pltpu.SemaphoreType.DMA((parts,)),
            pltpu.SemaphoreType.DMA((5, parts)),
            pltpu.SemaphoreType.DMA((parts,)),
            pltpu.SemaphoreType.DMA((1,)),
            pltpu.SemaphoreType.DMA((places,)),
            pltpu.SemaphoreType.DMA((1,)),
            pltpu.SemaphoreType.DMA((2 * groups,)),
        ],
        compiler_params=pltpu.CompilerParams(
            collective_id=0, has_side_effects=True, vmem_limit_bytes=grant
        ),
    )(pair_mask, log_scale, bias, image_emb, text_emb, positives)
    pieces = 4
    image_grad, text_grad = pl.pallas_call(
        functools.partial(store_kernel, pieces),
        out_shape=(
            jax.ShapeDtypeStruct(image_emb.shape, image_emb.dtype),
            jax.ShapeDtypeStruct(text_emb.shape, text_emb.dtype),
        ),
        in_specs=[vmem] * 2,
        out_specs=[pl.BlockSpec(memory_space=pltpu.HBM)] * 2,
        scratch_shapes=[pltpu.SemaphoreType.DMA((2, pieces))],
        compiler_params=pltpu.CompilerParams(vmem_limit_bytes=4 * 1024 * 1024),
    )(image_grad, text_grad)
    return image_grad, text_grad, loss


def solution(mesh):
    return jax.shard_map(
        body,
        mesh=mesh,
        in_specs=(
            P(("blk", "grp"), None),
            P(("blk", "grp"), None),
            P(("blk", "grp"), None),
            P(),
            P(),
            P(),
        ),
        out_specs=(P(("blk", "grp"), None), P(("blk", "grp"), None), P()),
        check_vma=False,
    )
```

```python
import functools

import jax
import jax.numpy as jnp
from jax import lax
from jax.experimental import pallas as pl
from jax.experimental.pallas import tpu as pltpu
from jax.sharding import PartitionSpec as P

epsilon = 1e-06


def passed_along(value, axis, steps):
    count = lax.axis_size(axis)
    pairs = [(source, (source + steps) % count) for source in range(count)]
    return lax.ppermute(value, axis, pairs)


def unit_rows(embedded):
    values = embedded.astype(jnp.float32)
    length = jnp.sqrt(jnp.sum(values * values, axis=1, keepdims=True) + epsilon)
    return (values / length, length)


def back_rows(normed, length, upstream):
    inward = jnp.sum(normed * upstream, axis=1, keepdims=True)
    return (upstream - normed * inward) / length


def score_tile(image_side, text_side, labels, logit_scale, offset):
    similar = jnp.einsum("rd,cd->rc", image_side, text_side, preferred_element_type=jnp.float32)
    logits = logit_scale * similar + offset
    signed = labels * logits
    loss_sum = jnp.sum(jax.nn.softplus(-signed))
    slopes = (-labels * jax.nn.sigmoid(-signed) * logit_scale).astype(jnp.bfloat16)
    return (slopes, loss_sum)


def masked_tile(active_flag, image_side, text_side, labels, logit_scale, offset):

    def active(unused):
        return score_tile(image_side, text_side, labels, logit_scale, offset)

    def skipped(unused):
        return (
            jnp.zeros((image_side.shape[0], text_side.shape[0]), jnp.bfloat16),
            jnp.zeros((), jnp.float32),
        )

    return lax.cond(active_flag > 0, active, skipped, 0)


def plain_body(image_emb, text_emb, positives, pair_mask, log_scale, bias):
    reach = (pair_mask.shape[1] - 1) // 2
    block_count = lax.axis_size("blk")
    myself = lax.axis_index("blk")
    logit_scale = jnp.exp(log_scale[0])
    offset = bias[0]
    row_count = image_emb.shape[0]
    image_normed, image_len = unit_rows(image_emb)
    text_normed, text_len = unit_rows(text_emb)
    image_half = image_normed.astype(jnp.bfloat16)
    text_half = text_normed.astype(jnp.bfloat16)
    columns = lax.broadcasted_iota(jnp.int32, (row_count, row_count), 1)
    own_labels = jnp.where(positives[0][:, None] == columns, 1.0, -1.0).astype(jnp.float32)
    apart_labels = -jnp.ones((row_count, row_count), jnp.float32)
    own_flags = lax.dynamic_index_in_dim(pair_mask, myself, 0, keepdims=False)
    fetched = {}
    for direction in (1, -1):
        moving = text_half
        for distance in range(1, reach + 1):
            moving = passed_along(moving, "blk", -direction)
            fetched[direction * distance] = moving
    slopes, loss_sum = masked_tile(
        own_flags[reach], image_half, text_half, own_labels, logit_scale, offset
    )
    image_total = jnp.dot(slopes, text_half, preferred_element_type=jnp.float32)
    text_total = jnp.einsum("rc,rd->cd", slopes, image_half, preferred_element_type=jnp.float32)
    for distance in range(-reach, reach + 1):
        if distance == 0:
            continue
        partner = fetched[distance]
        slopes, part_loss = masked_tile(
            own_flags[reach + distance], image_half, partner, apart_labels, logit_scale, offset
        )
        loss_sum = loss_sum + part_loss
        image_total = image_total + jnp.dot(slopes, partner, preferred_element_type=jnp.float32)
        partial_grad = jnp.einsum(
            "rc,rd->cd", slopes, image_half, preferred_element_type=jnp.float32
        ).astype(jnp.bfloat16)
        arrived = passed_along(partial_grad, "blk", distance)
        text_total = text_total + arrived.astype(jnp.float32)
    total_loss = lax.psum(loss_sum, ("blk", "grp"))
    image_count = row_count * block_count * lax.axis_size("grp")
    loss = (total_loss / image_count).reshape(1)
    image_grad = back_rows(image_normed, image_len, image_total).astype(jnp.bfloat16)
    text_grad = back_rows(text_normed, text_len, text_total).astype(jnp.bfloat16)
    return (image_grad, text_grad, loss)


MESH = pl.DeviceIdType.MESH
Y, INNER, OUTER = 0, 1, 2
OWN, OTHER = 0, 1


def grid_kernel(reach, parts, tiles, mask_hbm, scale_hbm, offset_hbm, image_hbm, text_hbm, pos_hbm,
                image_out, text_out, loss_out,
                mask_ref, scale_ref, offset_ref, loss_ref,
                texts, images, pos_row, unit_texts, unit_images, labels, slopes, terms, sent, got,
                image_acc, image_part, image_sent, image_got, loss_acc, line_loss, plane_loss,
                load_sem, send_sem, text_recv, image_recv, term_recv, back_recv,
                line_send, line_recv, plane_send, plane_recv):
    me = lax.axis_index("blk")
    grp = lax.axis_index("grp")
    count = lax.axis_size("blk")
    groups = lax.axis_size("grp")
    rows = images.shape[1]
    places = count // 2
    piece = rows // parts
    tall = rows // tiles
    per_tile = parts // tiles
    row, col = me // 2, me % 2
    top = row // 2
    role = row + top * (3 - 2 * row)
    toward = 1 - 2 * top
    aside = row * 2 + (1 - col)
    inner = (row + toward) * 2 + col
    outer = lax.rem((row - toward + 4), 4) * 2 + col
    targets = {Y: aside, INNER: inner, OUTER: outer}
    is_end, is_mid = role == 0, role == 1

    def place_row(p):
        return p + top * (3 - 2 * p)

    def cut(c):
        return pl.ds(pl.multiple_of(c * piece, piece), piece)

    def at(which, c):
        return pl.ds(pl.multiple_of(which * rows + c * piece, piece), piece)

    def tile_at(which, c):
        return pl.ds(pl.multiple_of(which * rows + c * tall, tall), tall)

    def send(way, slot, source, target, recv):
        return pltpu.make_async_remote_copy(
            src_ref=source, dst_ref=target, send_sem=send_sem.at[way, slot], recv_sem=recv,
            device_id=(targets[way], grp), device_id_type=MESH)

    def text_copy(way, slot, which, c):
        return send(way, slot, texts.at[at(which, c)], texts.at[at(which, c)], text_recv.at[which, c])

    def image_copy(c):
        return send(Y, 0, images.at[OWN, cut(c)], images.at[OTHER, cut(c)], image_recv.at[c])

    def back_copy(c):
        return send(Y, 1, image_sent.at[cut(c)], image_got.at[cut(c)], back_recv.at[c])

    def term_copy(way, slot, which, kind, c):
        return send(way, slot, sent.at[at(which, c)], got.at[kind, cut(c)], term_recv.at[kind, c])

    def term_arrived(kind, c):
        term_copy(INNER, 0, 0, kind, c).wait_recv()

    def all_sent(way, slot):
        block = texts.at[pl.ds(0, rows)]
        send(way, slot, block, block, text_recv.at[0, 0]).wait_send()

    own_row = place_row(role)
    loads = [
        pltpu.make_async_copy(source, target, load_sem.at[i])
        for i, (source, target) in enumerate((
            (text_hbm, texts.at[pl.ds(pl.multiple_of(own_row * rows, rows), rows)]),
            (image_hbm, images.at[OWN]), (pos_hbm, pos_row),
            (mask_hbm, mask_ref), (scale_hbm, scale_ref), (offset_hbm, offset_ref)))
    ]
    for load in loads:
        load.start()
    barrier = pltpu.get_barrier_semaphore()
    plane = 2 * groups
    spot = col * groups + grp

    def in_plane(d):
        other = lax.rem(spot + d, plane)
        return other, (row * 2 + other // groups, lax.rem(other, groups))

    pl.semaphore_signal(barrier, inc=1, device_id=(inner, grp), device_id_type=MESH)

    @pl.when(is_mid)
    def _():
        pl.semaphore_signal(barrier, inc=1, device_id=(outer, grp), device_id_type=MESH)

    @pl.loop(1, plane)
    def _(d):
        pl.semaphore_signal(barrier, inc=1, device_id=in_plane(d)[1], device_id_type=MESH)

    pl.semaphore_wait(barrier, plane + role)

    def line_share(d):
        target = lax.rem(row + d, places)
        return pltpu.make_async_remote_copy(
            src_ref=line_loss.at[row], dst_ref=line_loss.at[row], send_sem=line_send.at[0],
            recv_sem=line_recv.at[row], device_id=(target * 2 + col, grp), device_id_type=MESH)

    def line_arrival(d):
        source = lax.rem(row + d, places)
        return pltpu.make_async_remote_copy(
            src_ref=line_loss.at[source], dst_ref=line_loss.at[source], send_sem=line_send.at[0],
            recv_sem=line_recv.at[source], device_id=(source * 2 + col, grp), device_id_type=MESH)

    def plane_share(d):
        return pltpu.make_async_remote_copy(
            src_ref=plane_loss.at[spot], dst_ref=plane_loss.at[spot], send_sem=plane_send.at[0],
            recv_sem=plane_recv.at[spot], device_id=in_plane(d)[1], device_id_type=MESH)

    def plane_arrival(d):
        other, device = in_plane(d)
        return pltpu.make_async_remote_copy(
            src_ref=plane_loss.at[other], dst_ref=plane_loss.at[other], send_sem=plane_send.at[0],
            recv_sem=plane_recv.at[other], device_id=device, device_id_type=MESH)

    loads[0].wait()
    loads[1].wait()

    for load in loads[2:]:
        load.wait()

    scale = jnp.exp(jnp.full((1, 1), scale_ref[0], jnp.float32))
    offset = jnp.full((1, 1), offset_ref[0], jnp.float32)

    def unit(values):
        length = jnp.sqrt(jnp.sum(values * values, axis=1, keepdims=True) + epsilon)
        return values / length, length

    last_tile = tile_at(place_row(3 - 2 * role), tiles - 1)

    def prepare():
        loss_acc[...] = jnp.zeros_like(loss_acc)

        @pl.loop(0, tiles)
        def _(c):
            band = pl.ds(pl.multiple_of(c * tall, tall), tall)
            unit_images[band, :] = unit(images[OWN, band, :].astype(jnp.float32))[0].astype(jnp.bfloat16)
            hit = pos_row[...] == lax.broadcasted_iota(jnp.int32, (tall, rows), 0) + c * tall
            labels[1 + c] = jnp.transpose(jnp.where(hit, -1.0, 1.0))

        slopes[OTHER, :, last_tile] = jnp.zeros((rows, tall), jnp.bfloat16)
        unit_texts[last_tile, :] = jnp.zeros((tall, texts.shape[1]), jnp.bfloat16)
        labels[0] = jnp.full(labels.shape[1:], 1.0, jnp.float32)

    second = lax.rem(grp, 2)

    held = 1

    def image_arrived(c):
        image_copy(c).wait_recv()
        unit_images[at(1, c), :] = unit(images[OTHER, cut(c), :].astype(jnp.float32))[0].astype(jnp.bfloat16)

    def send_texts():
        @pl.loop(0, parts)
        def _(c):
            text_copy(INNER, 0, own_row, c).start()

            @pl.when(is_mid)
            def _():
                text_copy(OUTER, 0, own_row, c).start()

    def send_images():
        @pl.loop(0, parts)
        def _(c):
            image_copy(c).start()

    @pl.when(second == 0)
    def _():
        send_texts()

    send_images()
    prepare()

    @pl.when(second == 1)
    def _():
        @pl.loop(0, held)
        def _(c):
            image_arrived(c)

        send_texts()

    @pl.loop(0, parts)
    def _(c):
        @pl.when(is_mid)
        def _():
            text_copy(Y, 0, place_row(0), c).wait_recv()
            text_copy(INNER, 1, place_row(0), c).start()
            text_copy(Y, 0, place_row(2), c).wait_recv()
            text_copy(OUTER, 1, place_row(2), c).start()

        @pl.when(c // held + (1 - second) > 0)
        def _():
            image_arrived(c)

    def flag_of(other, which):
        image = row * 2 + col + other * (1 - 2 * col)
        text = which * 2 + col
        apart = lax.rem(text - image + reach + count, count)
        inside = 1 - apart // (2 * reach + 1)
        return (mask_ref[image, apart * inside] * inside).astype(jnp.float32)

    def item(p, which, c):
        text = unit(texts[tile_at(which, c), :].astype(jnp.float32))[0].astype(jnp.bfloat16)
        unit_texts[tile_at(which, c), :] = text
        own = 1 // (1 + (p - role) * (p - role))
        term = None
        for other in (OWN, OTHER):
            flag = flag_of(other, which)
            side = unit_images[other * rows:(other + 1) * rows, :]
            similar = lax.dot_general(side, text, (((1,), (1,)), ((), ())), preferred_element_type=jnp.float32)
            logits = scale * similar + offset
            factor = scale * flag
            if other == OWN:
                label = labels[(1 + c) * own]
                logits = logits * label
                factor = factor * label
            grown = jnp.exp(logits)
            lifted = 1.0 + grown
            slope = (grown / lifted * factor).astype(jnp.bfloat16)
            slopes[other, :, tile_at(which, c)] = slope
            loss_acc[...] += flag * jnp.sum(jnp.log(lifted), axis=0, keepdims=True)
            part = lax.dot_general(slope, side, (((0,), (0,)), ((), ())), preferred_element_type=jnp.float32)
            term = part if term is None else term + part
        terms[tile_at(which, c), :] = term
        sent[tile_at(which, c), :] = term.astype(jnp.bfloat16)

    def relay(way, slot, kind, p, onward, c):
        which = place_row(p)
        term_arrived(kind, c)
        total = terms[at(which, c), :] + got[kind, cut(c), :].astype(jnp.float32)
        sent[at(which, c), :] = total.astype(jnp.bfloat16)
        term_copy(way, slot, which, onward, c).start()

    steps = 4 * tiles

    @pl.loop(0, steps)
    def _(s):
        third = s // tiles
        first, last = (tiles - third) // tiles, third // tiles
        between, odd = 1 - first - last, (s + 1) % 2
        p = (first * (1 + role) + last * (3 - 2 * role)
             + between * ((1 - odd) * (2 - 2 * role) + odd * 3 * role))
        c = first * s + last * (s - 3 * tiles) + between * ((s + 1) // 2 - 2)
        which = place_row(p)

        @pl.when(s == steps - 1)
        def _():
            @pl.loop(0, tiles)
            def _(k):
                band = pl.ds(pl.multiple_of(k * tall, tall), tall)
                image_part[band, :] = jnp.dot(
                    slopes[OTHER, band, :], unit_texts[...], preferred_element_type=jnp.float32)

        @pl.when((1 - role) * p > 0)
        def _():
            @pl.loop(0, per_tile)
            def _(k):
                text_copy(Y, 0, which, c * per_tile + k).wait_recv()

        @pl.when(role * (p // 3) == 1)
        def _():
            @pl.loop(0, per_tile)
            def _(k):
                text_copy(Y, 0, which, c * per_tile + k).wait_recv()
                text_copy(OUTER, 2, which, c * per_tile + k).start()

        item(p, which, c)

        @pl.when(s == steps - 1)
        def _():
            line_loss[row] = jnp.full(line_loss.shape[1:], jnp.sum(loss_acc[...]), jnp.float32)

            @pl.loop(1, places)
            def _(d):
                line_share(d).start()

        @pl.when((1 - role) * (p // 2 + p % 2 * ((tiles - c) // tiles)) > 0)
        def _():
            @pl.loop(0, per_tile)
            def _(k):
                term_copy(INNER, p, which, p - 1, c * per_tile + k).start()

        @pl.when(role * (s // 6) * (1 - s // 11) == 1)
        def _():
            relay(INNER, 2, 1, 2, 3, s - 6)

    @pl.when(is_end)
    def _():
        @pl.loop(per_tile, parts)
        def _(k):
            term_copy(INNER, 1, place_row(1), 0, k).start()

    @pl.loop(0, parts)
    def _(c):
        @pl.when(is_mid)
        def _():
            relay(INNER, 3, 2, 3, 4, c)

        whole = image_part[cut(c), :] + jnp.dot(
            slopes[OTHER, cut(c), last_tile], unit_texts[last_tile, :], preferred_element_type=jnp.float32)
        image_sent[cut(c), :] = whole.astype(jnp.bfloat16)
        back_copy(c).start()
        image_acc[cut(c), :] = jnp.dot(
            slopes[OWN, cut(c), :], unit_texts[...], preferred_element_type=jnp.float32)

        @pl.when(role * c > 0)
        def _():
            relay(OUTER, 3, 4, 0, 3, c - 1)

        @pl.when(c == parts - 1)
        def _():
            @pl.loop(1, places)
            def _(d):
                line_arrival(d).wait_recv()

            plane_loss[spot] = jnp.sum(line_loss[...], axis=0)

            @pl.loop(1, plane)
            def _(d):
                plane_share(d).start()

    @pl.when(is_mid)
    def _():
        relay(OUTER, 3, 4, 0, 3, parts - 1)

        relay(INNER, 2, 1, 2, 3, parts - 1)

    def put_loss():
        return pltpu.make_async_copy(loss_ref, loss_out, load_sem.at[0])

    def finish(source, upstream, result, c):
        normed, length = unit(source.astype(jnp.float32))
        result[cut(c), :] = back_rows(normed, length, upstream).astype(result.dtype)

    @pl.loop(0, parts)
    def _(c):
        @pl.when(c == parts // 2)
        def _():
            @pl.loop(1, plane)
            def _(d):
                plane_arrival(d).wait_recv()

            total = jnp.sum(plane_loss[...], axis=0)
            loss_ref[0] = jnp.sum(total[0:1, 0:1]) / (rows * count * groups)
            put_loss().start()

        @pl.when(is_mid)
        def _():
            term_arrived(0, c)
            terms[at(own_row, c), :] += got[0, cut(c), :].astype(jnp.float32)

        term_arrived(3, c)
        total = terms[at(own_row, c), :] + got[3, cut(c), :].astype(jnp.float32)
        finish(texts[at(own_row, c), :], total, text_out, c)
        back_copy(c).wait_recv()
        total = image_acc[cut(c), :] + image_got[cut(c), :].astype(jnp.float32)
        finish(images[OWN, cut(c), :], total, image_out, c)

    put_loss().wait()
    lines = line_loss.at[pl.ds(0, places - 1)]
    pltpu.make_async_remote_copy(
        src_ref=lines, dst_ref=lines, send_sem=line_send.at[0], recv_sem=line_recv.at[0],
        device_id=(inner, grp), device_id_type=MESH).wait_send()
    planes = plane_loss.at[pl.ds(0, plane - 1)]
    pltpu.make_async_remote_copy(
        src_ref=planes, dst_ref=planes, send_sem=plane_send.at[0], recv_sem=plane_recv.at[0],
        device_id=(inner, grp), device_id_type=MESH).wait_send()
    for slot in range(2):
        all_sent(Y, slot)
    for slot in range(4):
        all_sent(INNER, slot)

    @pl.when(is_mid)
    def _():
        for slot in range(4):
            all_sent(OUTER, slot)


def store_kernel(pieces, image_ref, text_ref, image_out, text_out, sem):
    height = image_ref.shape[0] // pieces
    copies = [
        pltpu.make_async_copy(source.at[pl.ds(c * height, height)], result.at[pl.ds(c * height, height)], sem.at[i, c])
        for i, (source, result) in enumerate(((image_ref, image_out), (text_ref, text_out)))
        for c in range(pieces)
    ]
    for copy in copies:
        copy.start()
    for copy in copies:
        copy.wait()


def body(image_emb, text_emb, positives, pair_mask, log_scale, bias):
    reach = (pair_mask.shape[1] - 1) // 2
    block_count = lax.axis_size("blk")
    row_count, width = image_emb.shape
    if block_count != 2 * (reach + 1) or reach != 3 or row_count % (3 * 128) != 0:
        return plain_body(image_emb, text_emb, positives, pair_mask, log_scale, bias)
    parts, tiles = 6, 3
    places = block_count // 2
    groups = lax.axis_size("grp")
    vmem = pl.BlockSpec(memory_space=pltpu.VMEM)
    anywhere = pl.BlockSpec(memory_space=pl.ANY)
    column = places * row_count
    grant = 67043328 - 2 * image_emb.size * image_emb.dtype.itemsize
    image_grad, text_grad, loss = pl.pallas_call(
        functools.partial(grid_kernel, reach, parts, tiles),
        out_shape=(
            pltpu.VMEM(image_emb.shape, image_emb.dtype),
            pltpu.VMEM(text_emb.shape, text_emb.dtype),
            jax.ShapeDtypeStruct((1,), jnp.float32),
        ),
        in_specs=[pl.BlockSpec(memory_space=pltpu.HBM)] * 6,
        out_specs=(vmem, vmem, anywhere),
        scratch_shapes=[
            pltpu.SMEM(pair_mask.shape, jnp.int32),
            pltpu.SMEM((1,), jnp.float32),
            pltpu.SMEM((1,), jnp.float32),
            pltpu.SMEM((1,), jnp.float32),
            pltpu.VMEM((column, width), jnp.bfloat16),
            pltpu.VMEM((2, row_count, width), jnp.bfloat16),
            pltpu.VMEM((1, row_count), jnp.int32),
            pltpu.VMEM((column, width), jnp.bfloat16),
            pltpu.VMEM((2 * row_count, width), jnp.bfloat16),
            pltpu.VMEM((1 + tiles, row_count, row_count // tiles), jnp.float32),
            pltpu.VMEM((2, row_count, column), jnp.bfloat16),
            pltpu.VMEM((column, width), jnp.float32),
            pltpu.VMEM((column, width), jnp.bfloat16),
            pltpu.VMEM((5, row_count, width), jnp.bfloat16),
            pltpu.VMEM((row_count, width), jnp.float32),
            pltpu.VMEM((row_count, width), jnp.float32),
            pltpu.VMEM((row_count, width), jnp.bfloat16),
            pltpu.VMEM((row_count, width), jnp.bfloat16),
            pltpu.VMEM((1, row_count // tiles), jnp.float32),
            pltpu.VMEM((places, 8, 128), jnp.float32),
            pltpu.VMEM((2 * groups, 8, 128), jnp.float32),
            pltpu.SemaphoreType.DMA((6,)),
            pltpu.SemaphoreType.DMA((3, 4)),
            pltpu.SemaphoreType.DMA((places, parts)),
            pltpu.SemaphoreType.DMA((parts,)),
            pltpu.SemaphoreType.DMA((5, parts)),
            pltpu.SemaphoreType.DMA((parts,)),
            pltpu.SemaphoreType.DMA((1,)),
            pltpu.SemaphoreType.DMA((places,)),
            pltpu.SemaphoreType.DMA((1,)),
            pltpu.SemaphoreType.DMA((2 * groups,)),
        ],
        compiler_params=pltpu.CompilerParams(
            collective_id=0, has_side_effects=True, vmem_limit_bytes=grant
        ),
    )(pair_mask, log_scale, bias, image_emb, text_emb, positives)
    pieces = 4
    image_grad, text_grad = pl.pallas_call(
        functools.partial(store_kernel, pieces),
        out_shape=(
            jax.ShapeDtypeStruct(image_emb.shape, image_emb.dtype),
            jax.ShapeDtypeStruct(text_emb.shape, text_emb.dtype),
        ),
        in_specs=[vmem] * 2,
        out_specs=[pl.BlockSpec(memory_space=pltpu.HBM)] * 2,
        scratch_shapes=[pltpu.SemaphoreType.DMA((2, pieces))],
        compiler_params=pltpu.CompilerParams(vmem_limit_bytes=4 * 1024 * 1024),
    )(image_grad, text_grad)
    return image_grad, text_grad, loss


def solution(mesh):
    return jax.shard_map(
        body,
        mesh=mesh,
        in_specs=(
            P(("blk", "grp"), None),
            P(("blk", "grp"), None),
            P(("blk", "grp"), None),
            P(),
            P(),
            P(),
        ),
        out_specs=(P(("blk", "grp"), None), P(("blk", "grp"), None), P()),
        check_vma=False,
    )
```

```python
import functools

import jax
import jax.numpy as jnp
from jax import lax
from jax.experimental import pallas as pl
from jax.experimental.pallas import tpu as pltpu
from jax.sharding import PartitionSpec as P

epsilon = 1e-06


def passed_along(value, axis, steps):
    count = lax.axis_size(axis)
    pairs = [(source, (source + steps) % count) for source in range(count)]
    return lax.ppermute(value, axis, pairs)


def unit_rows(embedded):
    values = embedded.astype(jnp.float32)
    length = jnp.sqrt(jnp.sum(values * values, axis=1, keepdims=True) + epsilon)
    return (values / length, length)


def back_rows(normed, length, upstream):
    inward = jnp.sum(normed * upstream, axis=1, keepdims=True)
    return (upstream - normed * inward) / length


def score_tile(image_side, text_side, labels, logit_scale, offset):
    similar = jnp.einsum("rd,cd->rc", image_side, text_side, preferred_element_type=jnp.float32)
    logits = logit_scale * similar + offset
    signed = labels * logits
    loss_sum = jnp.sum(jax.nn.softplus(-signed))
    slopes = (-labels * jax.nn.sigmoid(-signed) * logit_scale).astype(jnp.bfloat16)
    return (slopes, loss_sum)


def masked_tile(active_flag, image_side, text_side, labels, logit_scale, offset):

    def active(unused):
        return score_tile(image_side, text_side, labels, logit_scale, offset)

    def skipped(unused):
        return (
            jnp.zeros((image_side.shape[0], text_side.shape[0]), jnp.bfloat16),
            jnp.zeros((), jnp.float32),
        )

    return lax.cond(active_flag > 0, active, skipped, 0)


def plain_body(image_emb, text_emb, positives, pair_mask, log_scale, bias):
    reach = (pair_mask.shape[1] - 1) // 2
    block_count = lax.axis_size("blk")
    myself = lax.axis_index("blk")
    logit_scale = jnp.exp(log_scale[0])
    offset = bias[0]
    row_count = image_emb.shape[0]
    image_normed, image_len = unit_rows(image_emb)
    text_normed, text_len = unit_rows(text_emb)
    image_half = image_normed.astype(jnp.bfloat16)
    text_half = text_normed.astype(jnp.bfloat16)
    columns = lax.broadcasted_iota(jnp.int32, (row_count, row_count), 1)
    own_labels = jnp.where(positives[0][:, None] == columns, 1.0, -1.0).astype(jnp.float32)
    apart_labels = -jnp.ones((row_count, row_count), jnp.float32)
    own_flags = lax.dynamic_index_in_dim(pair_mask, myself, 0, keepdims=False)
    fetched = {}
    for direction in (1, -1):
        moving = text_half
        for distance in range(1, reach + 1):
            moving = passed_along(moving, "blk", -direction)
            fetched[direction * distance] = moving
    slopes, loss_sum = masked_tile(
        own_flags[reach], image_half, text_half, own_labels, logit_scale, offset
    )
    image_total = jnp.dot(slopes, text_half, preferred_element_type=jnp.float32)
    text_total = jnp.einsum("rc,rd->cd", slopes, image_half, preferred_element_type=jnp.float32)
    for distance in range(-reach, reach + 1):
        if distance == 0:
            continue
        partner = fetched[distance]
        slopes, part_loss = masked_tile(
            own_flags[reach + distance], image_half, partner, apart_labels, logit_scale, offset
        )
        loss_sum = loss_sum + part_loss
        image_total = image_total + jnp.dot(slopes, partner, preferred_element_type=jnp.float32)
        partial_grad = jnp.einsum(
            "rc,rd->cd", slopes, image_half, preferred_element_type=jnp.float32
        ).astype(jnp.bfloat16)
        arrived = passed_along(partial_grad, "blk", distance)
        text_total = text_total + arrived.astype(jnp.float32)
    total_loss = lax.psum(loss_sum, ("blk", "grp"))
    image_count = row_count * block_count * lax.axis_size("grp")
    loss = (total_loss / image_count).reshape(1)
    image_grad = back_rows(image_normed, image_len, image_total).astype(jnp.bfloat16)
    text_grad = back_rows(text_normed, text_len, text_total).astype(jnp.bfloat16)
    return (image_grad, text_grad, loss)


MESH = pl.DeviceIdType.MESH
Y, INNER, OUTER = 0, 1, 2
OWN, OTHER = 0, 1


def grid_kernel(reach, parts, tiles, mask_hbm, scale_hbm, offset_hbm, image_hbm, text_hbm, pos_hbm,
                image_out, text_out, loss_out,
                mask_ref, scale_ref, offset_ref, loss_ref,
                texts, images, pos_row, unit_texts, unit_images, labels, slopes, terms, sent, got,
                image_acc, image_part, image_sent, image_got, loss_acc, line_loss, plane_loss,
                load_sem, send_sem, text_recv, image_recv, term_recv, back_recv,
                line_send, line_recv, plane_send, plane_recv):
    me = lax.axis_index("blk")
    grp = lax.axis_index("grp")
    count = lax.axis_size("blk")
    groups = lax.axis_size("grp")
    rows = images.shape[1]
    places = count // 2
    piece = rows // parts
    tall = rows // tiles
    per_tile = parts // tiles
    row, col = me // 2, me % 2
    top = row // 2
    role = row + top * (3 - 2 * row)
    toward = 1 - 2 * top
    aside = row * 2 + (1 - col)
    inner = (row + toward) * 2 + col
    outer = lax.rem((row - toward + 4), 4) * 2 + col
    targets = {Y: aside, INNER: inner, OUTER: outer}
    is_end, is_mid = role == 0, role == 1

    def place_row(p):
        return p + top * (3 - 2 * p)

    def cut(c):
        return pl.ds(pl.multiple_of(c * piece, piece), piece)

    def at(which, c):
        return pl.ds(pl.multiple_of(which * rows + c * piece, piece), piece)

    def tile_at(which, c):
        return pl.ds(pl.multiple_of(which * rows + c * tall, tall), tall)

    def send(way, slot, source, target, recv):
        return pltpu.make_async_remote_copy(
            src_ref=source, dst_ref=target, send_sem=send_sem.at[way, slot], recv_sem=recv,
            device_id=(targets[way], grp), device_id_type=MESH)

    def text_copy(way, slot, which, c):
        return send(way, slot, texts.at[at(which, c)], texts.at[at(which, c)], text_recv.at[which, c])

    def half_cut(i):
        return pl.ds(pl.multiple_of(i * (piece // 2), piece // 2), piece // 2)

    def image_copy(i):
        return send(Y, 0, images.at[OWN, half_cut(i)], images.at[OTHER, half_cut(i)], image_recv.at[i])

    def back_copy(c):
        return send(Y, 1, image_sent.at[cut(c)], image_got.at[cut(c)], back_recv.at[c])

    def term_copy(way, slot, which, kind, c):
        return send(way, slot, sent.at[at(which, c)], got.at[kind, cut(c)], term_recv.at[kind, c])

    def term_arrived(kind, c):
        term_copy(INNER, 0, 0, kind, c).wait_recv()

    def all_sent(way, slot):
        block = texts.at[pl.ds(0, rows)]
        send(way, slot, block, block, text_recv.at[0, 0]).wait_send()

    own_row = place_row(role)
    loads = [
        pltpu.make_async_copy(source, target, load_sem.at[i])
        for i, (source, target) in enumerate((
            (text_hbm, texts.at[pl.ds(pl.multiple_of(own_row * rows, rows), rows)]),
            (image_hbm, images.at[OWN]), (pos_hbm, pos_row),
            (mask_hbm, mask_ref), (scale_hbm, scale_ref), (offset_hbm, offset_ref)))
    ]
    for load in loads:
        load.start()
    barrier = pltpu.get_barrier_semaphore()
    plane = 2 * groups
    spot = col * groups + grp

    def in_plane(d):
        other = lax.rem(spot + d, plane)
        return other, (row * 2 + other // groups, lax.rem(other, groups))

    pl.semaphore_signal(barrier, inc=1, device_id=(inner, grp), device_id_type=MESH)

    @pl.when(is_mid)
    def _():
        pl.semaphore_signal(barrier, inc=1, device_id=(outer, grp), device_id_type=MESH)

    @pl.loop(1, plane)
    def _(d):
        pl.semaphore_signal(barrier, inc=1, device_id=in_plane(d)[1], device_id_type=MESH)

    pl.semaphore_wait(barrier, plane + role)

    def line_share(d):
        target = lax.rem(row + d, places)
        return pltpu.make_async_remote_copy(
            src_ref=line_loss.at[row], dst_ref=line_loss.at[row], send_sem=line_send.at[0],
            recv_sem=line_recv.at[row], device_id=(target * 2 + col, grp), device_id_type=MESH)

    def line_arrival(d):
        source = lax.rem(row + d, places)
        return pltpu.make_async_remote_copy(
            src_ref=line_loss.at[source], dst_ref=line_loss.at[source], send_sem=line_send.at[0],
            recv_sem=line_recv.at[source], device_id=(source * 2 + col, grp), device_id_type=MESH)

    def plane_share(d):
        return pltpu.make_async_remote_copy(
            src_ref=plane_loss.at[spot], dst_ref=plane_loss.at[spot], send_sem=plane_send.at[0],
            recv_sem=plane_recv.at[spot], device_id=in_plane(d)[1], device_id_type=MESH)

    def plane_arrival(d):
        other, device = in_plane(d)
        return pltpu.make_async_remote_copy(
            src_ref=plane_loss.at[other], dst_ref=plane_loss.at[other], send_sem=plane_send.at[0],
            recv_sem=plane_recv.at[other], device_id=device, device_id_type=MESH)

    loads[0].wait()
    loads[1].wait()

    for load in loads[2:]:
        load.wait()

    scale = jnp.exp(jnp.full((1, 1), scale_ref[0], jnp.float32))
    offset = jnp.full((1, 1), offset_ref[0], jnp.float32)

    def unit(values):
        length = jnp.sqrt(jnp.sum(values * values, axis=1, keepdims=True) + epsilon)
        return values / length, length

    last_tile = tile_at(place_row(3 - 2 * role), tiles - 1)

    def prepare():
        loss_acc[...] = jnp.zeros_like(loss_acc)

        @pl.loop(0, tiles)
        def _(c):
            band = pl.ds(pl.multiple_of(c * tall, tall), tall)
            unit_images[band, :] = unit(images[OWN, band, :].astype(jnp.float32))[0].astype(jnp.bfloat16)
            hit = pos_row[...] == lax.broadcasted_iota(jnp.int32, (tall, rows), 0) + c * tall
            labels[1 + c] = jnp.transpose(jnp.where(hit, -1.0, 1.0))

        slopes[OTHER, :, last_tile] = jnp.zeros((rows, tall), jnp.bfloat16)
        unit_texts[last_tile, :] = jnp.zeros((tall, texts.shape[1]), jnp.bfloat16)
        labels[0] = jnp.full(labels.shape[1:], 1.0, jnp.float32)

    second = lax.rem(grp, 2)

    early, held = 2, 5

    def image_arrived(i):
        image_copy(i).wait_recv()
        there = pl.ds(pl.multiple_of(rows + i * (piece // 2), piece // 2), piece // 2)
        unit_images[there, :] = unit(images[OTHER, half_cut(i), :].astype(jnp.float32))[0].astype(jnp.bfloat16)

    def send_texts(first, last):
        @pl.loop(first, last)
        def _(c):
            text_copy(INNER, 0, own_row, c).start()

            @pl.when(is_mid)
            def _():
                text_copy(OUTER, 0, own_row, c).start()

    send_texts(0, parts - second * (parts - early))

    @pl.loop(0, 2 * parts)
    def _(i):
        image_copy(i).start()

    prepare()

    @pl.when(second == 1)
    def _():
        @pl.loop(0, held)
        def _(c):
            image_arrived(c)

        send_texts(early, parts)

    @pl.loop(0, parts)
    def _(c):
        @pl.when(is_mid)
        def _():
            text_copy(Y, 0, place_row(0), c).wait_recv()
            text_copy(INNER, 1, place_row(0), c).start()
            text_copy(Y, 0, place_row(2), c).wait_recv()
            text_copy(OUTER, 1, place_row(2), c).start()

        @pl.loop(2 * c, 2 * c + 2)
        def _(i):
            @pl.when(i // held + (1 - second) > 0)
            def _():
                image_arrived(i)

    def flag_of(other, which):
        image = row * 2 + col + other * (1 - 2 * col)
        text = which * 2 + col
        apart = lax.rem(text - image + reach + count, count)
        inside = 1 - apart // (2 * reach + 1)
        return (mask_ref[image, apart * inside] * inside).astype(jnp.float32)

    def item(p, which, c):
        text = unit(texts[tile_at(which, c), :].astype(jnp.float32))[0].astype(jnp.bfloat16)
        unit_texts[tile_at(which, c), :] = text
        own = 1 // (1 + (p - role) * (p - role))
        term = None
        for other in (OWN, OTHER):
            flag = flag_of(other, which)
            side = unit_images[other * rows:(other + 1) * rows, :]
            similar = lax.dot_general(side, text, (((1,), (1,)), ((), ())), preferred_element_type=jnp.float32)
            logits = scale * similar + offset
            factor = scale * flag
            if other == OWN:
                label = labels[(1 + c) * own]
                logits = logits * label
                factor = factor * label
            grown = jnp.exp(logits)
            lifted = 1.0 + grown
            slope = (grown / lifted * factor).astype(jnp.bfloat16)
            slopes[other, :, tile_at(which, c)] = slope
            loss_acc[...] += flag * jnp.sum(jnp.log(lifted), axis=0, keepdims=True)
            part = lax.dot_general(slope, side, (((0,), (0,)), ((), ())), preferred_element_type=jnp.float32)
            term = part if term is None else term + part
        terms[tile_at(which, c), :] = term
        sent[tile_at(which, c), :] = term.astype(jnp.bfloat16)

    def relay(way, slot, kind, p, onward, c):
        which = place_row(p)
        term_arrived(kind, c)
        total = terms[at(which, c), :] + got[kind, cut(c), :].astype(jnp.float32)
        sent[at(which, c), :] = total.astype(jnp.bfloat16)
        term_copy(way, slot, which, onward, c).start()

    steps = 4 * tiles

    @pl.loop(0, steps)
    def _(s):
        third = s // tiles
        first, last = (tiles - third) // tiles, third // tiles
        between, odd = 1 - first - last, (s + 1) % 2
        p = (first * (1 + role) + last * (3 - 2 * role)
             + between * ((1 - odd) * (2 - 2 * role) + odd * 3 * role))
        c = first * s + last * (s - 3 * tiles) + between * ((s + 1) // 2 - 2)
        which = place_row(p)

        @pl.when(s == steps - 1)
        def _():
            @pl.loop(0, tiles)
            def _(k):
                band = pl.ds(pl.multiple_of(k * tall, tall), tall)
                image_part[band, :] = jnp.dot(
                    slopes[OTHER, band, :], unit_texts[...], preferred_element_type=jnp.float32)

        @pl.when((1 - role) * p > 0)
        def _():
            @pl.loop(0, per_tile)
            def _(k):
                text_copy(Y, 0, which, c * per_tile + k).wait_recv()

        @pl.when(role * (p // 3) == 1)
        def _():
            @pl.loop(0, per_tile)
            def _(k):
                text_copy(Y, 0, which, c * per_tile + k).wait_recv()
                text_copy(OUTER, 2, which, c * per_tile + k).start()

        item(p, which, c)

        @pl.when(s == steps - 1)
        def _():
            line_loss[row] = jnp.full(line_loss.shape[1:], jnp.sum(loss_acc[...]), jnp.float32)

            @pl.loop(1, places)
            def _(d):
                line_share(d).start()

        @pl.when((1 - role) * (p // 2 + p % 2 * ((tiles - c) // tiles)) > 0)
        def _():
            @pl.loop(0, per_tile)
            def _(k):
                term_copy(INNER, p, which, p - 1, c * per_tile + k).start()

        @pl.when(role * (s // 6) * (1 - s // 11) == 1)
        def _():
            relay(INNER, 2, 1, 2, 3, s - 6)

    @pl.when(is_end)
    def _():
        @pl.loop(per_tile, parts)
        def _(k):
            term_copy(INNER, 1, place_row(1), 0, k).start()

    @pl.loop(0, parts)
    def _(c):
        @pl.when(is_mid)
        def _():
            relay(INNER, 3, 2, 3, 4, c)

        whole = image_part[cut(c), :] + jnp.dot(
            slopes[OTHER, cut(c), last_tile], unit_texts[last_tile, :], preferred_element_type=jnp.float32)
        image_sent[cut(c), :] = whole.astype(jnp.bfloat16)
        back_copy(c).start()
        image_acc[cut(c), :] = jnp.dot(
            slopes[OWN, cut(c), :], unit_texts[...], preferred_element_type=jnp.float32)

        @pl.when(role * c > 0)
        def _():
            relay(OUTER, 3, 4, 0, 3, c - 1)

        @pl.when(c == parts - 1)
        def _():
            @pl.loop(1, places)
            def _(d):
                line_arrival(d).wait_recv()

            plane_loss[spot] = jnp.sum(line_loss[...], axis=0)

            @pl.loop(1, plane)
            def _(d):
                plane_share(d).start()

    @pl.when(is_mid)
    def _():
        relay(OUTER, 3, 4, 0, 3, parts - 1)

        relay(INNER, 2, 1, 2, 3, parts - 1)

    def put_loss():
        return pltpu.make_async_copy(loss_ref, loss_out, load_sem.at[0])

    def finish(source, upstream, result, c):
        normed, length = unit(source.astype(jnp.float32))
        result[cut(c), :] = back_rows(normed, length, upstream).astype(result.dtype)

    @pl.loop(0, parts)
    def _(c):
        @pl.when(c == parts // 2)
        def _():
            @pl.loop(1, plane)
            def _(d):
                plane_arrival(d).wait_recv()

            total = jnp.sum(plane_loss[...], axis=0)
            loss_ref[0] = jnp.sum(total[0:1, 0:1]) / (rows * count * groups)
            put_loss().start()

        @pl.when(is_mid)
        def _():
            term_arrived(0, c)
            terms[at(own_row, c), :] += got[0, cut(c), :].astype(jnp.float32)

        term_arrived(3, c)
        total = terms[at(own_row, c), :] + got[3, cut(c), :].astype(jnp.float32)
        finish(texts[at(own_row, c), :], total, text_out, c)
        back_copy(c).wait_recv()
        total = image_acc[cut(c), :] + image_got[cut(c), :].astype(jnp.float32)
        finish(images[OWN, cut(c), :], total, image_out, c)

    put_loss().wait()
    lines = line_loss.at[pl.ds(0, places - 1)]
    pltpu.make_async_remote_copy(
        src_ref=lines, dst_ref=lines, send_sem=line_send.at[0], recv_sem=line_recv.at[0],
        device_id=(inner, grp), device_id_type=MESH).wait_send()
    planes = plane_loss.at[pl.ds(0, plane - 1)]
    pltpu.make_async_remote_copy(
        src_ref=planes, dst_ref=planes, send_sem=plane_send.at[0], recv_sem=plane_recv.at[0],
        device_id=(inner, grp), device_id_type=MESH).wait_send()
    for slot in range(2):
        all_sent(Y, slot)
    for slot in range(4):
        all_sent(INNER, slot)

    @pl.when(is_mid)
    def _():
        for slot in range(4):
            all_sent(OUTER, slot)


def store_kernel(pieces, image_ref, text_ref, image_out, text_out, sem):
    height = image_ref.shape[0] // pieces
    copies = [
        pltpu.make_async_copy(source.at[pl.ds(c * height, height)], result.at[pl.ds(c * height, height)], sem.at[i, c])
        for i, (source, result) in enumerate(((image_ref, image_out), (text_ref, text_out)))
        for c in range(pieces)
    ]
    for copy in copies:
        copy.start()
    for copy in copies:
        copy.wait()


def body(image_emb, text_emb, positives, pair_mask, log_scale, bias):
    reach = (pair_mask.shape[1] - 1) // 2
    block_count = lax.axis_size("blk")
    row_count, width = image_emb.shape
    if block_count != 2 * (reach + 1) or reach != 3 or row_count % (3 * 128) != 0:
        return plain_body(image_emb, text_emb, positives, pair_mask, log_scale, bias)
    parts, tiles = 6, 3
    places = block_count // 2
    groups = lax.axis_size("grp")
    vmem = pl.BlockSpec(memory_space=pltpu.VMEM)
    anywhere = pl.BlockSpec(memory_space=pl.ANY)
    column = places * row_count
    grant = 67043328 - 2 * image_emb.size * image_emb.dtype.itemsize
    image_grad, text_grad, loss = pl.pallas_call(
        functools.partial(grid_kernel, reach, parts, tiles),
        out_shape=(
            pltpu.VMEM(image_emb.shape, image_emb.dtype),
            pltpu.VMEM(text_emb.shape, text_emb.dtype),
            jax.ShapeDtypeStruct((1,), jnp.float32),
        ),
        in_specs=[pl.BlockSpec(memory_space=pltpu.HBM)] * 6,
        out_specs=(vmem, vmem, anywhere),
        scratch_shapes=[
            pltpu.SMEM(pair_mask.shape, jnp.int32),
            pltpu.SMEM((1,), jnp.float32),
            pltpu.SMEM((1,), jnp.float32),
            pltpu.SMEM((1,), jnp.float32),
            pltpu.VMEM((column, width), jnp.bfloat16),
            pltpu.VMEM((2, row_count, width), jnp.bfloat16),
            pltpu.VMEM((1, row_count), jnp.int32),
            pltpu.VMEM((column, width), jnp.bfloat16),
            pltpu.VMEM((2 * row_count, width), jnp.bfloat16),
            pltpu.VMEM((1 + tiles, row_count, row_count // tiles), jnp.float32),
            pltpu.VMEM((2, row_count, column), jnp.bfloat16),
            pltpu.VMEM((column, width), jnp.float32),
            pltpu.VMEM((column, width), jnp.bfloat16),
            pltpu.VMEM((5, row_count, width), jnp.bfloat16),
            pltpu.VMEM((row_count, width), jnp.float32),
            pltpu.VMEM((row_count, width), jnp.float32),
            pltpu.VMEM((row_count, width), jnp.bfloat16),
            pltpu.VMEM((row_count, width), jnp.bfloat16),
            pltpu.VMEM((1, row_count // tiles), jnp.float32),
            pltpu.VMEM((places, 8, 128), jnp.float32),
            pltpu.VMEM((2 * groups, 8, 128), jnp.float32),
            pltpu.SemaphoreType.DMA((6,)),
            pltpu.SemaphoreType.DMA((3, 4)),
            pltpu.SemaphoreType.DMA((places, parts)),
            pltpu.SemaphoreType.DMA((2 * parts,)),
            pltpu.SemaphoreType.DMA((5, parts)),
            pltpu.SemaphoreType.DMA((parts,)),
            pltpu.SemaphoreType.DMA((1,)),
            pltpu.SemaphoreType.DMA((places,)),
            pltpu.SemaphoreType.DMA((1,)),
            pltpu.SemaphoreType.DMA((2 * groups,)),
        ],
        compiler_params=pltpu.CompilerParams(
            collective_id=0, has_side_effects=True, vmem_limit_bytes=grant
        ),
    )(pair_mask, log_scale, bias, image_emb, text_emb, positives)
    pieces = 4
    image_grad, text_grad = pl.pallas_call(
        functools.partial(store_kernel, pieces),
        out_shape=(
            jax.ShapeDtypeStruct(image_emb.shape, image_emb.dtype),
            jax.ShapeDtypeStruct(text_emb.shape, text_emb.dtype),
        ),
        in_specs=[vmem] * 2,
        out_specs=[pl.BlockSpec(memory_space=pltpu.HBM)] * 2,
        scratch_shapes=[pltpu.SemaphoreType.DMA((2, pieces))],
        compiler_params=pltpu.CompilerParams(vmem_limit_bytes=4 * 1024 * 1024),
    )(image_grad, text_grad)
    return image_grad, text_grad, loss


def solution(mesh):
    return jax.shard_map(
        body,
        mesh=mesh,
        in_specs=(
            P(("blk", "grp"), None),
            P(("blk", "grp"), None),
            P(("blk", "grp"), None),
            P(),
            P(),
            P(),
        ),
        out_specs=(P(("blk", "grp"), None), P(("blk", "grp"), None), P()),
        check_vma=False,
    )
```

```python
import functools

import jax
import jax.numpy as jnp
from jax import lax
from jax.experimental import pallas as pl
from jax.experimental.pallas import tpu as pltpu
from jax.sharding import PartitionSpec as P

epsilon = 1e-06


def passed_along(value, axis, steps):
    count = lax.axis_size(axis)
    pairs = [(source, (source + steps) % count) for source in range(count)]
    return lax.ppermute(value, axis, pairs)


def unit_rows(embedded):
    values = embedded.astype(jnp.float32)
    length = jnp.sqrt(jnp.sum(values * values, axis=1, keepdims=True) + epsilon)
    return (values / length, length)


def back_rows(normed, length, upstream):
    inward = jnp.sum(normed * upstream, axis=1, keepdims=True)
    return (upstream - normed * inward) / length


def score_tile(image_side, text_side, labels, logit_scale, offset):
    similar = jnp.einsum("rd,cd->rc", image_side, text_side, preferred_element_type=jnp.float32)
    logits = logit_scale * similar + offset
    signed = labels * logits
    loss_sum = jnp.sum(jax.nn.softplus(-signed))
    slopes = (-labels * jax.nn.sigmoid(-signed) * logit_scale).astype(jnp.bfloat16)
    return (slopes, loss_sum)


def masked_tile(active_flag, image_side, text_side, labels, logit_scale, offset):

    def active(unused):
        return score_tile(image_side, text_side, labels, logit_scale, offset)

    def skipped(unused):
        return (
            jnp.zeros((image_side.shape[0], text_side.shape[0]), jnp.bfloat16),
            jnp.zeros((), jnp.float32),
        )

    return lax.cond(active_flag > 0, active, skipped, 0)


def plain_body(image_emb, text_emb, positives, pair_mask, log_scale, bias):
    reach = (pair_mask.shape[1] - 1) // 2
    block_count = lax.axis_size("blk")
    myself = lax.axis_index("blk")
    logit_scale = jnp.exp(log_scale[0])
    offset = bias[0]
    row_count = image_emb.shape[0]
    image_normed, image_len = unit_rows(image_emb)
    text_normed, text_len = unit_rows(text_emb)
    image_half = image_normed.astype(jnp.bfloat16)
    text_half = text_normed.astype(jnp.bfloat16)
    columns = lax.broadcasted_iota(jnp.int32, (row_count, row_count), 1)
    own_labels = jnp.where(positives[0][:, None] == columns, 1.0, -1.0).astype(jnp.float32)
    apart_labels = -jnp.ones((row_count, row_count), jnp.float32)
    own_flags = lax.dynamic_index_in_dim(pair_mask, myself, 0, keepdims=False)
    fetched = {}
    for direction in (1, -1):
        moving = text_half
        for distance in range(1, reach + 1):
            moving = passed_along(moving, "blk", -direction)
            fetched[direction * distance] = moving
    slopes, loss_sum = masked_tile(
        own_flags[reach], image_half, text_half, own_labels, logit_scale, offset
    )
    image_total = jnp.dot(slopes, text_half, preferred_element_type=jnp.float32)
    text_total = jnp.einsum("rc,rd->cd", slopes, image_half, preferred_element_type=jnp.float32)
    for distance in range(-reach, reach + 1):
        if distance == 0:
            continue
        partner = fetched[distance]
        slopes, part_loss = masked_tile(
            own_flags[reach + distance], image_half, partner, apart_labels, logit_scale, offset
        )
        loss_sum = loss_sum + part_loss
        image_total = image_total + jnp.dot(slopes, partner, preferred_element_type=jnp.float32)
        partial_grad = jnp.einsum(
            "rc,rd->cd", slopes, image_half, preferred_element_type=jnp.float32
        ).astype(jnp.bfloat16)
        arrived = passed_along(partial_grad, "blk", distance)
        text_total = text_total + arrived.astype(jnp.float32)
    total_loss = lax.psum(loss_sum, ("blk", "grp"))
    image_count = row_count * block_count * lax.axis_size("grp")
    loss = (total_loss / image_count).reshape(1)
    image_grad = back_rows(image_normed, image_len, image_total).astype(jnp.bfloat16)
    text_grad = back_rows(text_normed, text_len, text_total).astype(jnp.bfloat16)
    return (image_grad, text_grad, loss)


MESH = pl.DeviceIdType.MESH
Y, INNER, OUTER = 0, 1, 2
OWN, OTHER = 0, 1


def grid_kernel(reach, parts, tiles, mask_hbm, scale_hbm, offset_hbm, image_hbm, text_hbm, pos_hbm,
                image_out, text_out, loss_out,
                mask_ref, scale_ref, offset_ref, loss_ref,
                texts, images, pos_row, unit_texts, unit_images, labels, slopes, terms, sent, got,
                image_acc, image_part, image_sent, image_got, loss_acc, line_loss, plane_loss,
                load_sem, send_sem, text_recv, image_recv, term_recv, back_recv,
                line_send, line_recv, plane_send, plane_recv):
    me = lax.axis_index("blk")
    grp = lax.axis_index("grp")
    count = lax.axis_size("blk")
    groups = lax.axis_size("grp")
    rows = images.shape[1]
    places = count // 2
    piece = rows // parts
    tall = rows // tiles
    per_tile = parts // tiles
    row, col = me // 2, me % 2
    top = row // 2
    role = row + top * (3 - 2 * row)
    toward = 1 - 2 * top
    aside = row * 2 + (1 - col)
    inner = (row + toward) * 2 + col
    outer = lax.rem((row - toward + 4), 4) * 2 + col
    targets = {Y: aside, INNER: inner, OUTER: outer}
    is_end, is_mid = role == 0, role == 1

    def place_row(p):
        return p + top * (3 - 2 * p)

    def cut(c):
        return pl.ds(pl.multiple_of(c * piece, piece), piece)

    def at(which, c):
        return pl.ds(pl.multiple_of(which * rows + c * piece, piece), piece)

    def tile_at(which, c):
        return pl.ds(pl.multiple_of(which * rows + c * tall, tall), tall)

    def send(way, slot, source, target, recv):
        return pltpu.make_async_remote_copy(
            src_ref=source, dst_ref=target, send_sem=send_sem.at[way, slot], recv_sem=recv,
            device_id=(targets[way], grp), device_id_type=MESH)

    def text_copy(way, slot, which, c):
        return send(way, slot, texts.at[at(which, c)], texts.at[at(which, c)], text_recv.at[which, c])

    def half_cut(i):
        return pl.ds(pl.multiple_of(i * (piece // 2), piece // 2), piece // 2)

    def image_copy(i):
        return send(Y, 0, images.at[OWN, half_cut(i)], images.at[OTHER, half_cut(i)], image_recv.at[i])

    def back_copy(c):
        return send(Y, 1, image_sent.at[cut(c)], image_got.at[cut(c)], back_recv.at[c])

    def term_copy(way, slot, which, kind, c):
        return send(way, slot, sent.at[at(which, c)], got.at[kind, cut(c)], term_recv.at[kind, c])

    def term_arrived(kind, c):
        term_copy(INNER, 0, 0, kind, c).wait_recv()

    def all_sent(way, slot):
        block = texts.at[pl.ds(0, rows)]
        send(way, slot, block, block, text_recv.at[0, 0]).wait_send()

    own_row = place_row(role)
    loads = [
        pltpu.make_async_copy(source, target, load_sem.at[i])
        for i, (source, target) in enumerate((
            (image_hbm, images.at[OWN]), (pos_hbm, pos_row),
            (mask_hbm, mask_ref), (scale_hbm, scale_ref), (offset_hbm, offset_ref)))
    ]

    def text_load(c):
        return pltpu.make_async_copy(text_hbm.at[cut(c)], texts.at[at(own_row, c)], load_sem.at[len(loads) + c])

    @pl.loop(0, parts)
    def _(c):
        text_load(c).start()

    for load in loads:
        load.start()
    barrier = pltpu.get_barrier_semaphore()
    plane = 2 * groups
    spot = col * groups + grp

    def in_plane(d):
        other = lax.rem(spot + d, plane)
        return other, (row * 2 + other // groups, lax.rem(other, groups))

    pl.semaphore_signal(barrier, inc=1, device_id=(inner, grp), device_id_type=MESH)

    @pl.when(is_mid)
    def _():
        pl.semaphore_signal(barrier, inc=1, device_id=(outer, grp), device_id_type=MESH)

    @pl.loop(1, plane)
    def _(d):
        pl.semaphore_signal(barrier, inc=1, device_id=in_plane(d)[1], device_id_type=MESH)

    pl.semaphore_wait(barrier, plane + role)

    def line_share(d):
        target = lax.rem(row + d, places)
        return pltpu.make_async_remote_copy(
            src_ref=line_loss.at[row], dst_ref=line_loss.at[row], send_sem=line_send.at[0],
            recv_sem=line_recv.at[row], device_id=(target * 2 + col, grp), device_id_type=MESH)

    def line_arrival(d):
        source = lax.rem(row + d, places)
        return pltpu.make_async_remote_copy(
            src_ref=line_loss.at[source], dst_ref=line_loss.at[source], send_sem=line_send.at[0],
            recv_sem=line_recv.at[source], device_id=(source * 2 + col, grp), device_id_type=MESH)

    def plane_share(d):
        return pltpu.make_async_remote_copy(
            src_ref=plane_loss.at[spot], dst_ref=plane_loss.at[spot], send_sem=plane_send.at[0],
            recv_sem=plane_recv.at[spot], device_id=in_plane(d)[1], device_id_type=MESH)

    def plane_arrival(d):
        other, device = in_plane(d)
        return pltpu.make_async_remote_copy(
            src_ref=plane_loss.at[other], dst_ref=plane_loss.at[other], send_sem=plane_send.at[0],
            recv_sem=plane_recv.at[other], device_id=device, device_id_type=MESH)

    def unit(values):
        length = jnp.sqrt(jnp.sum(values * values, axis=1, keepdims=True) + epsilon)
        return values / length, length

    last_tile = tile_at(place_row(3 - 2 * role), tiles - 1)

    def prepare():
        loss_acc[...] = jnp.zeros_like(loss_acc)

        @pl.loop(0, tiles)
        def _(c):
            band = pl.ds(pl.multiple_of(c * tall, tall), tall)
            unit_images[band, :] = unit(images[OWN, band, :].astype(jnp.float32))[0].astype(jnp.bfloat16)
            hit = pos_row[...] == lax.broadcasted_iota(jnp.int32, (tall, rows), 0) + c * tall
            labels[1 + c] = jnp.transpose(jnp.where(hit, -1.0, 1.0))

        slopes[OTHER, :, last_tile] = jnp.zeros((rows, tall), jnp.bfloat16)
        unit_texts[last_tile, :] = jnp.zeros((tall, texts.shape[1]), jnp.bfloat16)
        labels[0] = jnp.full(labels.shape[1:], 1.0, jnp.float32)

    second = lax.rem(grp, 2)

    early, held = 2, 5

    def image_arrived(i):
        image_copy(i).wait_recv()
        there = pl.ds(pl.multiple_of(rows + i * (piece // 2), piece // 2), piece // 2)
        unit_images[there, :] = unit(images[OTHER, half_cut(i), :].astype(jnp.float32))[0].astype(jnp.bfloat16)

    def send_texts(first, last):
        @pl.loop(first, last)
        def _(c):
            text_load(c).wait()
            text_copy(INNER, 0, own_row, c).start()

            @pl.when(is_mid)
            def _():
                text_copy(OUTER, 0, own_row, c).start()

    send_texts(0, parts - second * (parts - early))

    loads[0].wait()

    @pl.loop(0, 2 * parts)
    def _(i):
        image_copy(i).start()

    for load in loads[1:]:
        load.wait()

    scale = jnp.exp(jnp.full((1, 1), scale_ref[0], jnp.float32))
    offset = jnp.full((1, 1), offset_ref[0], jnp.float32)

    prepare()

    @pl.when(second == 1)
    def _():
        @pl.loop(0, held)
        def _(c):
            image_arrived(c)

        send_texts(early, parts)

    @pl.loop(0, parts)
    def _(c):
        @pl.when(is_mid)
        def _():
            text_copy(Y, 0, place_row(0), c).wait_recv()
            text_copy(INNER, 1, place_row(0), c).start()
            text_copy(Y, 0, place_row(2), c).wait_recv()
            text_copy(OUTER, 1, place_row(2), c).start()

        @pl.loop(2 * c, 2 * c + 2)
        def _(i):
            @pl.when(i // held + (1 - second) > 0)
            def _():
                image_arrived(i)

    def flag_of(other, which):
        image = row * 2 + col + other * (1 - 2 * col)
        text = which * 2 + col
        apart = lax.rem(text - image + reach + count, count)
        inside = 1 - apart // (2 * reach + 1)
        return (mask_ref[image, apart * inside] * inside).astype(jnp.float32)

    def item(p, which, c):
        text = unit(texts[tile_at(which, c), :].astype(jnp.float32))[0].astype(jnp.bfloat16)
        unit_texts[tile_at(which, c), :] = text
        own = 1 // (1 + (p - role) * (p - role))
        term = None
        for other in (OWN, OTHER):
            flag = flag_of(other, which)
            side = unit_images[other * rows:(other + 1) * rows, :]
            similar = lax.dot_general(side, text, (((1,), (1,)), ((), ())), preferred_element_type=jnp.float32)
            logits = scale * similar + offset
            factor = scale * flag
            if other == OWN:
                label = labels[(1 + c) * own]
                logits = logits * label
                factor = factor * label
            grown = jnp.exp(logits)
            lifted = 1.0 + grown
            slope = (grown / lifted * factor).astype(jnp.bfloat16)
            slopes[other, :, tile_at(which, c)] = slope
            loss_acc[...] += flag * jnp.sum(jnp.log(lifted), axis=0, keepdims=True)
            part = lax.dot_general(slope, side, (((0,), (0,)), ((), ())), preferred_element_type=jnp.float32)
            term = part if term is None else term + part
        terms[tile_at(which, c), :] = term
        sent[tile_at(which, c), :] = term.astype(jnp.bfloat16)

    def relay(way, slot, kind, p, onward, c):
        which = place_row(p)
        term_arrived(kind, c)
        total = terms[at(which, c), :] + got[kind, cut(c), :].astype(jnp.float32)
        sent[at(which, c), :] = total.astype(jnp.bfloat16)
        term_copy(way, slot, which, onward, c).start()

    steps = 4 * tiles

    @pl.loop(0, steps)
    def _(s):
        third = s // tiles
        first, last = (tiles - third) // tiles, third // tiles
        between, odd = 1 - first - last, (s + 1) % 2
        p = (first * (1 + role) + last * (3 - 2 * role)
             + between * ((1 - odd) * (2 - 2 * role) + odd * 3 * role))
        c = first * s + last * (s - 3 * tiles) + between * ((s + 1) // 2 - 2)
        which = place_row(p)

        @pl.when((1 - role) * (s + 1) == steps)
        def _():
            @pl.loop(0, tiles)
            def _(k):
                band = pl.ds(pl.multiple_of(k * tall, tall), tall)
                image_part[band, :] = jnp.dot(
                    slopes[OTHER, band, :], unit_texts[...], preferred_element_type=jnp.float32)

        @pl.when((1 - role) * p > 0)
        def _():
            @pl.loop(0, per_tile)
            def _(k):
                text_copy(Y, 0, which, c * per_tile + k).wait_recv()

        @pl.when(role * (p // 3) == 1)
        def _():
            @pl.loop(0, per_tile)
            def _(k):
                text_copy(Y, 0, which, c * per_tile + k).wait_recv()
                text_copy(OUTER, 2, which, c * per_tile + k).start()

        item(p, which, c)

        @pl.when(s == steps - 1)
        def _():
            line_loss[row] = jnp.full(line_loss.shape[1:], jnp.sum(loss_acc[...]), jnp.float32)

            @pl.loop(1, places)
            def _(d):
                line_share(d).start()

        @pl.when((1 - role) * (p // 2 + p % 2 * ((tiles - c) // tiles)) > 0)
        def _():
            @pl.loop(0, per_tile)
            def _(k):
                term_copy(INNER, p, which, p - 1, c * per_tile + k).start()

        @pl.when(role * (s // 6) * (1 - s // 11) == 1)
        def _():
            relay(INNER, 2, 1, 2, 3, s - 6)

    @pl.when(is_end)
    def _():
        @pl.loop(per_tile, parts)
        def _(k):
            term_copy(INNER, 1, place_row(1), 0, k).start()

    @pl.loop(0, parts)
    def _(c):
        @pl.when(is_mid)
        def _():
            relay(INNER, 3, 2, 3, 4, c)

        @pl.when(is_end)
        def _():
            whole = image_part[cut(c), :] + jnp.dot(
                slopes[OTHER, cut(c), last_tile], unit_texts[last_tile, :], preferred_element_type=jnp.float32)
            image_sent[cut(c), :] = whole.astype(jnp.bfloat16)

        @pl.when(is_mid)
        def _():
            whole = jnp.dot(slopes[OTHER, cut(c), :], unit_texts[...], preferred_element_type=jnp.float32)
            image_sent[cut(c), :] = whole.astype(jnp.bfloat16)

        back_copy(c).start()
        image_acc[cut(c), :] = jnp.dot(
            slopes[OWN, cut(c), :], unit_texts[...], preferred_element_type=jnp.float32)

        @pl.when(role * c > 0)
        def _():
            relay(OUTER, 3, 4, 0, 3, c - 1)

        @pl.when(c == parts - 1)
        def _():
            @pl.loop(1, places)
            def _(d):
                line_arrival(d).wait_recv()

            plane_loss[spot] = jnp.sum(line_loss[...], axis=0)

            @pl.loop(1, plane)
            def _(d):
                plane_share(d).start()

    @pl.when(is_mid)
    def _():
        relay(OUTER, 3, 4, 0, 3, parts - 1)

        relay(INNER, 2, 1, 2, 3, parts - 1)

    def put_loss():
        return pltpu.make_async_copy(loss_ref, loss_out, load_sem.at[0])

    def finish(source, upstream, result, c):
        normed, length = unit(source.astype(jnp.float32))
        result[cut(c), :] = back_rows(normed, length, upstream).astype(result.dtype)

    @pl.loop(0, parts)
    def _(c):
        @pl.when(c == parts // 2)
        def _():
            @pl.loop(1, plane)
            def _(d):
                plane_arrival(d).wait_recv()

            total = jnp.sum(plane_loss[...], axis=0)
            loss_ref[0] = jnp.sum(total[0:1, 0:1]) / (rows * count * groups)
            put_loss().start()

        @pl.when(is_mid)
        def _():
            term_arrived(0, c)
            terms[at(own_row, c), :] += got[0, cut(c), :].astype(jnp.float32)

        term_arrived(3, c)
        total = terms[at(own_row, c), :] + got[3, cut(c), :].astype(jnp.float32)
        finish(texts[at(own_row, c), :], total, text_out, c)
        back_copy(c).wait_recv()
        total = image_acc[cut(c), :] + image_got[cut(c), :].astype(jnp.float32)
        finish(images[OWN, cut(c), :], total, image_out, c)

    put_loss().wait()
    lines = line_loss.at[pl.ds(0, places - 1)]
    pltpu.make_async_remote_copy(
        src_ref=lines, dst_ref=lines, send_sem=line_send.at[0], recv_sem=line_recv.at[0],
        device_id=(inner, grp), device_id_type=MESH).wait_send()
    planes = plane_loss.at[pl.ds(0, plane - 1)]
    pltpu.make_async_remote_copy(
        src_ref=planes, dst_ref=planes, send_sem=plane_send.at[0], recv_sem=plane_recv.at[0],
        device_id=(inner, grp), device_id_type=MESH).wait_send()
    for slot in range(2):
        all_sent(Y, slot)
    for slot in range(4):
        all_sent(INNER, slot)

    @pl.when(is_mid)
    def _():
        for slot in range(4):
            all_sent(OUTER, slot)


def store_kernel(pieces, image_ref, text_ref, image_out, text_out, sem):
    height = image_ref.shape[0] // pieces
    copies = [
        pltpu.make_async_copy(source.at[pl.ds(c * height, height)], result.at[pl.ds(c * height, height)], sem.at[i, c])
        for i, (source, result) in enumerate(((image_ref, image_out), (text_ref, text_out)))
        for c in range(pieces)
    ]
    for copy in copies:
        copy.start()
    for copy in copies:
        copy.wait()


def body(image_emb, text_emb, positives, pair_mask, log_scale, bias):
    reach = (pair_mask.shape[1] - 1) // 2
    block_count = lax.axis_size("blk")
    row_count, width = image_emb.shape
    if block_count != 2 * (reach + 1) or reach != 3 or row_count % (3 * 128) != 0:
        return plain_body(image_emb, text_emb, positives, pair_mask, log_scale, bias)
    parts, tiles = 6, 3
    places = block_count // 2
    groups = lax.axis_size("grp")
    vmem = pl.BlockSpec(memory_space=pltpu.VMEM)
    anywhere = pl.BlockSpec(memory_space=pl.ANY)
    column = places * row_count
    grant = 67043328 - 2 * image_emb.size * image_emb.dtype.itemsize
    image_grad, text_grad, loss = pl.pallas_call(
        functools.partial(grid_kernel, reach, parts, tiles),
        out_shape=(
            pltpu.VMEM(image_emb.shape, image_emb.dtype),
            pltpu.VMEM(text_emb.shape, text_emb.dtype),
            jax.ShapeDtypeStruct((1,), jnp.float32),
        ),
        in_specs=[pl.BlockSpec(memory_space=pltpu.HBM)] * 6,
        out_specs=(vmem, vmem, anywhere),
        scratch_shapes=[
            pltpu.SMEM(pair_mask.shape, jnp.int32),
            pltpu.SMEM((1,), jnp.float32),
            pltpu.SMEM((1,), jnp.float32),
            pltpu.SMEM((1,), jnp.float32),
            pltpu.VMEM((column, width), jnp.bfloat16),
            pltpu.VMEM((2, row_count, width), jnp.bfloat16),
            pltpu.VMEM((1, row_count), jnp.int32),
            pltpu.VMEM((column, width), jnp.bfloat16),
            pltpu.VMEM((2 * row_count, width), jnp.bfloat16),
            pltpu.VMEM((1 + tiles, row_count, row_count // tiles), jnp.float32),
            pltpu.VMEM((2, row_count, column), jnp.bfloat16),
            pltpu.VMEM((column, width), jnp.float32),
            pltpu.VMEM((column, width), jnp.bfloat16),
            pltpu.VMEM((5, row_count, width), jnp.bfloat16),
            pltpu.VMEM((row_count, width), jnp.float32),
            pltpu.VMEM((row_count, width), jnp.float32),
            pltpu.VMEM((row_count, width), jnp.bfloat16),
            pltpu.VMEM((row_count, width), jnp.bfloat16),
            pltpu.VMEM((1, row_count // tiles), jnp.float32),
            pltpu.VMEM((places, 8, 128), jnp.float32),
            pltpu.VMEM((2 * groups, 8, 128), jnp.float32),
            pltpu.SemaphoreType.DMA((5 + parts,)),
            pltpu.SemaphoreType.DMA((3, 4)),
            pltpu.SemaphoreType.DMA((places, parts)),
            pltpu.SemaphoreType.DMA((2 * parts,)),
            pltpu.SemaphoreType.DMA((5, parts)),
            pltpu.SemaphoreType.DMA((parts,)),
            pltpu.SemaphoreType.DMA((1,)),
            pltpu.SemaphoreType.DMA((places,)),
            pltpu.SemaphoreType.DMA((1,)),
            pltpu.SemaphoreType.DMA((2 * groups,)),
        ],
        compiler_params=pltpu.CompilerParams(
            collective_id=0, has_side_effects=True, vmem_limit_bytes=grant
        ),
    )(pair_mask, log_scale, bias, image_emb, text_emb, positives)
    pieces = 4
    image_grad, text_grad = pl.pallas_call(
        functools.partial(store_kernel, pieces),
        out_shape=(
            jax.ShapeDtypeStruct(image_emb.shape, image_emb.dtype),
            jax.ShapeDtypeStruct(text_emb.shape, text_emb.dtype),
        ),
        in_specs=[vmem] * 2,
        out_specs=[pl.BlockSpec(memory_space=pltpu.HBM)] * 2,
        scratch_shapes=[pltpu.SemaphoreType.DMA((2, pieces))],
        compiler_params=pltpu.CompilerParams(vmem_limit_bytes=4 * 1024 * 1024),
    )(image_grad, text_grad)
    return image_grad, text_grad, loss


def solution(mesh):
    return jax.shard_map(
        body,
        mesh=mesh,
        in_specs=(
            P(("blk", "grp"), None),
            P(("blk", "grp"), None),
            P(("blk", "grp"), None),
            P(),
            P(),
            P(),
        ),
        out_specs=(P(("blk", "grp"), None), P(("blk", "grp"), None), P()),
        check_vma=False,
    )
```
